128 devices in a mesh: rows: 8 (over x, core), cols: 16 (over y, z).
Axes of the slice: x: 4, y: 4, z: 4, core: 2. Of those that a mesh axis runs over, the one named last changes fastest.
Arguments:
- slab: float32 [65536, 2048], P('rows', 'cols'), may hold values from -6 to 6
- sign_bits: int32 [65536], P('rows'), may hold values from 0 to 1
- sample_rows: int32 [8192], replicated, may hold values from 0 to 65535, as said below
Outputs:
- gram: float32 [2048, 2048], P('rows', 'cols')
The draws below stay inside these ranges and needn't reach their ends.
Inputs may be any that keep to these rules, and one draw needn't show every extreme that they name: `sample_rows`: Ascending; repeats may occur. At most 2048 indices fall in any one device's aligned block of 8192 rows, and some block holds exactly 2048.
All inputs are finite; a program needn't handle non-finite values.
Results may differ from the reference program's by a relative error of at most 0.000071.
Values sent between devices are 32-bit elements; how exact they have to be, the bound alone decides.
A program may use at most 64 MiB of HBM per device.

```python
import jax
import jax.numpy as jnp
from jax import lax

D = 2048
ROWS_DEV = 8192
SAMP = 1024
M = 65536
SAMPLES = 8192
N_ROWS = 8


def draw_sample_rows(key, part):
    first_key, second_key, third_key = jax.random.split(key, 3)
    pairs = N_ROWS // 2
    excess = jax.random.randint(first_key, (pairs,), 0, SAMP + 1).astype(jnp.int32)
    excess = excess.at[0].set(SAMP)
    paired = jnp.stack([SAMP + excess, SAMP - excess], axis=1).reshape(N_ROWS)
    ordering = jax.random.permutation(second_key, N_ROWS)
    counts = paired[ordering]
    bounds = jnp.cumsum(counts).astype(jnp.int32)
    slot_ids = jnp.arange(SAMPLES, dtype=jnp.int32)
    owners = jnp.sum((slot_ids[:, None] >= bounds[None, :]).astype(jnp.int32), axis=1).astype(jnp.int32)
    offset = jax.random.randint(third_key, (SAMPLES,), 0, ROWS_DEV).astype(jnp.int32)
    return jnp.sort(owners * ROWS_DEV + offset).astype(jnp.int32)


def plant(drawn, rng, least, top_value):
    index_at = [jax.random.randint(jax.random.fold_in(rng, axis), (), 0, length) for axis, length in enumerate(drawn.shape)]
    widest = drawn.shape.index(max(drawn.shape))
    neighbour = index_at[:widest] + [(index_at[widest] + 1) % drawn.shape[widest]] + index_at[widest + 1:]
    return drawn.at[tuple(index_at)].set(least).at[tuple(neighbour)].set(top_value)


def block_scale(own_key, dims, shards, low, high):
    factor_of = 1.0
    for axis_at, shards_of in shards:
        heights = jax.random.uniform(jax.random.fold_in(jax.random.fold_in(own_key, 6), axis_at), (shards_of,), jnp.float32, low / len(shards), high / len(shards))
        factor_of = factor_of * jnp.repeat(jnp.exp(heights), dims[axis_at] // shards_of).reshape((-1,) + (1,) * (len(dims) - 1 - axis_at))
    return factor_of


def normal_values(rng, extent, scale, reach, shards=(), kind=jnp.bfloat16):
    values = scale * jax.random.normal(rng, extent, jnp.float32)
    if shards:
        values = values * block_scale(rng, extent, shards, -0.22, 0.18)
    return jnp.clip(values, -reach, reach).astype(kind)


def setup_inputs(seed: int = 0) -> dict:
    seeds = jax.random.split(jax.random.key(seed), 4)
    slab = normal_values(seeds[0], (M, D), 1.0, 6.0, ((0, 8), (1, 16)), jnp.float32)
    sign_bits = plant(jax.random.randint(seeds[1], (M,), 0, 2), jax.random.fold_in(seeds[1], 1), 0, 1).astype(jnp.int32)
    sample_rows = draw_sample_rows(jax.random.fold_in(seeds[3], 71), 0)
    return dict(slab=slab, sign_bits=sign_bits, sample_rows=sample_rows)


def parity_table(length):
    index_list = jnp.arange(length, dtype=jnp.int32)
    common = index_list[:, None] & index_list[None, :]
    parity = jnp.zeros((length, length), jnp.int32)
    for bit_number in range(max(length.bit_length() - 1, 0)):
        parity = parity + ((common >> bit_number) & 1)
    return (1 - 2 * (parity % 2)).astype(jnp.float32)


def reference(slab, sign_bits, sample_rows):
    flipped = slab * (1 - 2 * sign_bits).astype(jnp.float32)[:, None]
    blocks = flipped.reshape(M // 128, 128, D)
    mixed = jnp.einsum("ij,qjc->qic", parity_table(128), blocks, precision=lax.Precision.HIGHEST)
    outer_count = M // 128
    stride = 1
    while stride < outer_count:
        shaped = mixed.reshape(outer_count // (2 * stride), 2, stride, 128, D)
        first_half = shaped[:, 0]
        second_half = shaped[:, 1]
        mixed = jnp.stack([first_half + second_half, first_half - second_half], axis=1)
        stride = stride * 2
    mixed = mixed.reshape(M, D)
    picked = jnp.take(mixed, sample_rows, axis=0)
    gram = jnp.dot(picked.T, picked, precision=lax.Precision.HIGHEST, preferred_element_type=jnp.float32)
    return gram * (1.0 / (SAMPLES * M))
```

```python
import jax
import jax.numpy as jnp
from jax import lax
from jax.sharding import PartitionSpec as P


def parity_table(length):
    index_list = jnp.arange(length, dtype=jnp.int32)
    common = index_list[:, None] & index_list[None, :]
    parity = jnp.zeros((length, length), jnp.int32)
    for bit_number in range(max(length.bit_length() - 1, 0)):
        parity = parity + (common >> bit_number & 1)
    return (1 - 2 * (parity % 2)).astype(jnp.float32)


def local_transform(slab, sign_bits):
    height, columns = slab.shape
    flipped = slab * (1 - 2 * sign_bits).astype(jnp.float32)[:, None]
    blocks = flipped.reshape(height // 128, 128, columns)
    inside = jnp.einsum("ij,qjc->qic", parity_table(128), blocks, precision=lax.Precision.HIGHEST)
    outside = jnp.einsum(
        "pq,qic->pic", parity_table(height // 128), inside, precision=lax.Precision.HIGHEST
    )
    return outside.reshape(height, columns)


def column_product(portion, own_rows):
    return lax.dot_general(
        portion,
        own_rows,
        (((0,), (0,)), ((), ())),
        precision=lax.Precision.HIGHEST,
        preferred_element_type=jnp.float32,
    )


def shards(slab, sign_bits, sample_rows):
    local = local_transform(slab, sign_bits)
    height = local.shape[0]
    groups = lax.axis_size("rows")
    me = lax.axis_index("rows")
    samples = sample_rows.shape[0]
    factor = 1.0 / (samples * height * groups)
    offsets = sample_rows % height
    common = (sample_rows // height) & me
    parity = (common ^ common >> 1 ^ common >> 2) & 1
    terms = jnp.take(local, offsets, axis=0) * (1 - 2 * parity).astype(jnp.float32)[:, None]
    picked = lax.psum_scatter(terms, "rows", scatter_dimension=0, tiled=True)
    gram = column_product(lax.all_gather(picked, "cols", axis=1, tiled=True), picked)
    return lax.psum_scatter(gram * factor, "rows", scatter_dimension=0, tiled=True)


def solution(mesh):
    return jax.shard_map(
        shards,
        mesh=mesh,
        in_specs=(P("rows", "cols"), P("rows"), P()),
        out_specs=P("rows", "cols"),
        check_vma=False,
    )
```

```python
import functools

import jax
import jax.numpy as jnp
from jax import lax
from jax.experimental import pallas as pl
from jax.experimental.pallas import tpu as pltpu
from jax.sharding import PartitionSpec as P

HEIGHT = 8192
SLOTS = 1024
GROUPS = 4
STEP = SLOTS // GROUPS
HALF = STEP // 2
WIDE = 128
MESH = pl.DeviceIdType.MESH


def parity_of(bits):
    bits = bits ^ (bits >> 4)
    bits = bits ^ (bits >> 2)
    bits = bits ^ (bits >> 1)
    return bits & 1


def split(value):
    high = value.astype(jnp.bfloat16)
    low = (value - high.astype(jnp.float32)).astype(jnp.bfloat16)
    return high, low


def kernel(
    codes, signs, slab, out,
    raw, table, mine, theirs, from_core, from_x1, from_x2, ybuf, zbuf,
    gram, core_gram, pieces, relay, arrive1, arrive2,
    load_sem, d_send, d_recv, x1_send, x1_recv, x2_send, x2_recv,
    y_send, y_recv, yf_send, yf_recv, z_send, z_recv, zf_send, zf_recv,
    c1_send, c1_recv, c2_send, c2_recv, c3_send, c3_recv,
):
    row = lax.axis_index("rows")
    col = lax.axis_index("cols")
    x, k = row // 2, row % 2
    y, z = col // 4, col % 4
    partner = (row + 1 - 2 * k, col)
    x_next = (((x + 1) % 4) * 2 + k, col)
    x_prev = (((x + 3) % 4) * 2 + k, col)
    y_next = (row, ((y + 1) % 4) * 4 + z)
    y_prev = (row, ((y + 3) % 4) * 4 + z)
    z_next = (row, y * 4 + (z + 1) % 4)
    z_prev = (row, y * 4 + (z + 3) % 4)

    loads = []
    for part in range(8):
        rows = pl.ds(part * 1024, 1024)
        loads.append(pltpu.make_async_copy(slab.at[rows], raw.at[rows], load_sem.at[part]))
        loads[-1].start()

    barrier = pltpu.get_barrier_semaphore()
    for other in (partner, x_next, x_prev, y_next, y_prev, z_next, z_prev):
        pl.semaphore_signal(barrier, inc=1, device_id=other, device_id_type=MESH)

    left = lax.broadcasted_iota(jnp.int32, (256, 256), 0)
    right = lax.broadcasted_iota(jnp.int32, (256, 256), 1)
    hadamard = (1 - 2 * parity_of(left & right)).astype(jnp.float32)

    def inside(q, carry):
        lower = hadamard[:, :128] * signs[pl.ds(2 * q, 1), :]
        upper = hadamard[:, 128:] * signs[pl.ds(2 * q + 1, 1), :]
        matrix = jnp.concatenate([lower, upper], axis=1).astype(jnp.bfloat16)
        start = pl.multiple_of(q * 256, 256)
        high, low = split(raw[pl.ds(start, 256), :])
        both = jnp.dot(
            matrix, jnp.concatenate([high, low], axis=1), preferred_element_type=jnp.float32
        )
        table[pl.ds(start, 256), :] = both[:, :128] + both[:, 128:]
        return carry

    for part in range(8):
        loads[part].wait()
        lax.fori_loop(part * 4, part * 4 + 4, inside, 0)

    def across(t, carry):
        starts = [pl.multiple_of(q * 256 + t * 8, 8) for q in range(32)]
        values = [table[pl.ds(start, 8), :] for start in starts]
        span = 1
        while span < 32:
            for base in range(0, 32, 2 * span):
                for i in range(base, base + span):
                    first, second = values[i], values[i + span]
                    values[i], values[i + span] = first + second, first - second
            span *= 2
        for start, value in zip(starts, values):
            table[pl.ds(start, 8), :] = value
            table[pl.ds(start + HEIGHT, 8), :] = -value
        return carry

    lax.fori_loop(0, 32, across, 0)

    pl.semaphore_wait(barrier, 7)

    def gather(g, d, core, target):
        base = (((x + d) % 4) * 2 + core) * SLOTS + g * STEP

        def eight(i, carry):
            at = pl.multiple_of(i * 8, 8)
            for u in range(8):
                target[pl.ds(at + u, 1), :] = table[pl.ds(codes[base + at + u], 1), :]
            return carry

        lax.fori_loop(0, STEP // 8, eight, 0)

    def remote(source, target, send, recv, device):
        return pltpu.make_async_remote_copy(
            src_ref=source, dst_ref=target, send_sem=send, recv_sem=recv,
            device_id=device, device_id_type=MESH,
        )

    sent = []

    def go(copy):
        copy.start()
        sent.append(copy)

    first, last = pl.ds(0, HALF), pl.ds(HALF, HALF)
    upper, lower = pl.ds(0, 64), pl.ds(64, 64)

    def core_copy(g, d):
        return remote(theirs.at[g, d], from_core.at[g, d], d_send.at[g, d], d_recv.at[g, d], partner)

    def x1_copy(g, side):
        rows, device = ((first, x_prev), (last, x_next))[side]
        return remote(
            mine.at[g, 2, rows], from_x1.at[g, side], x1_send.at[g, side], x1_recv.at[g, side], device
        )

    def x2_copy(g, side):
        d, device = ((3, x_prev), (1, x_next))[side]
        return remote(
            mine.at[g, d], from_x2.at[g, side], x2_send.at[g, side], x2_recv.at[g, side], device
        )

    def y_copy(g, side):
        device = (y_prev, y_next)[side]
        return remote(ybuf.at[g, y], ybuf.at[g, y], y_send.at[g, side], y_recv.at[g, side], device)

    def y_arrival(g, side):
        block = ((y + 1) % 4, (y + 3) % 4)[side]
        return remote(
            ybuf.at[g, block], ybuf.at[g, block], y_send.at[g, side], y_recv.at[g, side],
            (y_prev, y_next)[side],
        )

    def y_forward(g, side):
        block = ((y + 1) % 4, (y + 3) % 4)[side]
        rows, device = ((last, y_prev), (first, y_next))[side]
        return remote(
            ybuf.at[g, block, rows], ybuf.at[g, block, rows],
            yf_send.at[g, side], yf_recv.at[g, side], device,
        )

    def z_copy(g, side):
        device = (z_prev, z_next)[side]
        return remote(zbuf.at[g, z], zbuf.at[g, z], z_send.at[g, side], z_recv.at[g, side], device)

    def z_arrival(g, side):
        block = ((z + 1) % 4, (z + 3) % 4)[side]
        return remote(
            zbuf.at[g, block], zbuf.at[g, block], z_send.at[g, side], z_recv.at[g, side],
            (z_prev, z_next)[side],
        )

    def z_forward(g, side):
        block = ((z + 1) % 4, (z + 3) % 4)[side]
        rows, device = ((lower, z_prev), (upper, z_next))[side]
        return remote(
            zbuf.at[g, block, rows], zbuf.at[g, block, rows],
            zf_send.at[g, side], zf_recv.at[g, side], device,
        )

    def y_forwarded(g, side):
        rows = (last, first)[side]
        block = (y + 2) % 4
        return remote(
            ybuf.at[g, block, rows], ybuf.at[g, block, rows],
            yf_send.at[g, side], yf_recv.at[g, side], (y_prev, y_next)[side],
        )

    def z_forwarded(g, side):
        rows = (lower, upper)[side]
        block = (z + 2) % 4
        return remote(
            zbuf.at[g, block, rows], zbuf.at[g, block, rows],
            zf_send.at[g, side], zf_recv.at[g, side], (z_prev, z_next)[side],
        )

    def gather_one(g, d):
        gather(g, d, 1 - k, theirs.at[g, d])
        go(core_copy(g, d))
        gather(g, d, k, mine.at[g, d])

    def step1(g):
        gather_one(g, 2)
        core_copy(g, 2).wait_recv()
        mine[g, 2] = mine[g, 2] + from_core[g, 2]
        go(x1_copy(g, 0))
        go(x1_copy(g, 1))
        for d in (3, 1, 0):
            gather_one(g, d)

    def step2(g):
        x1_copy(g, 0).wait_recv()
        core_copy(g, 3).wait_recv()
        mine[g, 3, first] = mine[g, 3, first] + from_core[g, 3, first] + from_x1[g, 0]
        mine[g, 3, last] = mine[g, 3, last] + from_core[g, 3, last]
        go(x2_copy(g, 0))
        x1_copy(g, 1).wait_recv()
        core_copy(g, 1).wait_recv()
        mine[g, 1, first] = mine[g, 1, first] + from_core[g, 1, first]
        mine[g, 1, last] = mine[g, 1, last] + from_core[g, 1, last] + from_x1[g, 1]
        go(x2_copy(g, 1))

    def step3(g):
        core_copy(g, 0).wait_recv()
        x2_copy(g, 0).wait_recv()
        x2_copy(g, 1).wait_recv()
        block = mine[g, 0] + from_core[g, 0] + from_x2[g, 0] + from_x2[g, 1]
        ybuf[g, y] = block
        zbuf[g, z] = block.T
        go(y_copy(g, 0))
        go(y_copy(g, 1))
        go(z_copy(g, 0))
        go(z_copy(g, 1))

    def step4(g):
        for side in range(2):
            y_arrival(g, side).wait_recv()
            go(y_forward(g, side))
            z_arrival(g, side).wait_recv()
            go(z_forward(g, side))

    def step5(g):
        for side in range(2):
            y_forwarded(g, side).wait_recv()
            z_forwarded(g, side).wait_recv()
        for m in range(2):
            lhs = [split(zbuf[g, 2 * m + i]) for i in range(2)]
            lhs_high = jnp.concatenate([lhs[0][0], lhs[1][0]], axis=0)
            lhs_low = jnp.concatenate([lhs[0][1], lhs[1][1]], axis=0)
            for n in range(2):
                rhs = [split(ybuf[g, 2 * n + i]) for i in range(2)]
                rhs_high = jnp.concatenate([rhs[0][0], rhs[1][0]], axis=1)
                rhs_low = jnp.concatenate([rhs[0][1], rhs[1][1]], axis=1)
                product = functools.partial(jnp.dot, preferred_element_type=jnp.float32)
                value = (
                    product(lhs_high, rhs_high)
                    + product(lhs_high, rhs_low)
                    + product(lhs_low, rhs_high)
                )
                for i in range(2):
                    part = value[:, i * 128:(i + 1) * 128]
                    if g:
                        part = part + gram[2 * n + i, pl.ds(m * 256, 256), :]
                    gram[2 * n + i, pl.ds(m * 256, 256), :] = part

    stages = (step1, step2, step3, step4, step5)
    for turn in range(GROUPS + len(stages) - 1):
        for late, stage in enumerate(stages):
            if 0 <= turn - late < GROUPS:
                stage(turn - late)

    own_rows = pl.ds(pl.multiple_of(k * 256, 256), 256)
    other_rows = pl.ds(pl.multiple_of((1 - k) * 256, 256), 256)

    def c1_copy(d):
        at = (y + d) % 4
        return remote(gram.at[at, other_rows], core_gram.at[at], c1_send.at[d], c1_recv.at[d], partner)

    for d in (2, 3, 1, 0):
        go(c1_copy(d))

    def combined(d):
        c1_copy(d).wait_recv()
        at = (y + d) % 4
        gram[at, own_rows] = gram[at, own_rows] + core_gram[at]

    rows0, rows1 = pl.ds(0, 128), pl.ds(128, 128)
    k_rows = [
        pl.ds(pl.multiple_of(k * 256, 256), 128),
        pl.ds(pl.multiple_of(k * 256 + 128, 128), 128),
    ]

    def relay_copy(side):
        return remote(
            gram.at[(y + 2) % 4, k_rows[side]], relay.at[side],
            c2_send.at[side], c2_recv.at[side], (y_prev, y_next)[side],
        )

    def relay_on(side):
        block = ((y + 1) % 4, (y + 3) % 4)[side]
        return remote(
            relay.at[side], pieces.at[block, (rows0, rows1)[side]],
            c2_send.at[2 + side], c2_recv.at[2 + side], (y_prev, y_next)[side],
        )

    def relayed(side):
        return remote(
            relay.at[side], pieces.at[(y + 2) % 4, (rows0, rows1)[side]],
            c2_send.at[2 + side], c2_recv.at[2 + side], (y_prev, y_next)[side],
        )

    def near_copy(side):
        at = ((y + 3) % 4, (y + 1) % 4)[side]
        return remote(
            gram.at[at, own_rows], pieces.at[y],
            c2_send.at[4 + side], c2_recv.at[4 + side], (y_prev, y_next)[side],
        )

    def near_arrival(side):
        return remote(
            gram.at[y, own_rows], pieces.at[((y + 1) % 4, (y + 3) % 4)[side]],
            c2_send.at[4 + side], c2_recv.at[4 + side], (y_prev, y_next)[side],
        )

    combined(2)
    go(relay_copy(0))
    go(relay_copy(1))
    combined(3)
    go(near_copy(0))
    combined(1)
    go(near_copy(1))
    for side in range(2):
        relay_copy(side).wait_recv()
        go(relay_on(side))
    c1_copy(0).wait_recv()
    pieces[y] = gram[y, own_rows] + core_gram[y]
    for side in range(2):
        near_arrival(side).wait_recv()
    for side in range(2):
        relayed(side).wait_recv()

    def c3_first(side):
        return remote(
            pieces.at[(x + 2) % 4, (rows0, rows1)[side]], arrive1.at[side],
            c3_send.at[side], c3_recv.at[side], (x_prev, x_next)[side],
        )

    def c3_second(side):
        return remote(
            pieces.at[((x + 3) % 4, (x + 1) % 4)[side]], arrive2.at[side],
            c3_send.at[2 + side], c3_recv.at[2 + side], (x_prev, x_next)[side],
        )

    for side in range(2):
        go(c3_first(side))
    for side in range(2):
        c3_first(side).wait_recv()
        at = ((x + 3) % 4, (x + 1) % 4)[side]
        rows = (rows0, rows1)[side]
        pieces[at, rows] = pieces[at, rows] + arrive1[side]
        go(c3_second(side))
    for side in range(2):
        c3_second(side).wait_recv()
    out[...] = (pieces[x] + arrive2[0] + arrive2[1]) * (1.0 / (8 * SLOTS * 8 * HEIGHT))

    for copy in sent:
        copy.wait_send()


def shards(slab, sign_bits, sample_rows):
    me = lax.axis_index("rows")
    parity = parity_of((sample_rows // HEIGHT) & me)
    codes = sample_rows % HEIGHT + HEIGHT * parity
    signs = (1 - 2 * sign_bits).astype(jnp.float32).reshape(64, 128)
    dma = pltpu.SemaphoreType.DMA
    f32 = functools.partial(pltpu.VMEM, dtype=jnp.float32)
    vmem = lambda *shape: pltpu.VMEM(shape, jnp.float32)
    return pl.pallas_call(
        kernel,
        out_shape=jax.ShapeDtypeStruct((256, 128), jnp.float32),
        in_specs=[
            pl.BlockSpec(memory_space=pltpu.SMEM),
            pl.BlockSpec(memory_space=pltpu.VMEM),
            pl.BlockSpec(memory_space=pl.ANY),
        ],
        out_specs=pl.BlockSpec(memory_space=pltpu.VMEM),
        scratch_shapes=[
            vmem(HEIGHT, WIDE),
            vmem(2 * HEIGHT, WIDE),
            vmem(GROUPS, 4, STEP, WIDE),
            vmem(GROUPS, 4, STEP, WIDE),
            vmem(GROUPS, 4, STEP, WIDE),
            vmem(GROUPS, 2, HALF, WIDE),
            vmem(GROUPS, 2, STEP, WIDE),
            vmem(GROUPS, 4, STEP, WIDE),
            vmem(GROUPS, 4, WIDE, STEP),
            vmem(4, 512, WIDE),
            vmem(4, 256, WIDE),
            vmem(4, 256, WIDE),
            vmem(2, 128, WIDE),
            vmem(2, 128, WIDE),
            vmem(2, 256, WIDE),
            dma((8,)),
            dma((GROUPS, 4)), dma((GROUPS, 4)),
            dma((GROUPS, 2)), dma((GROUPS, 2)),
            dma((GROUPS, 2)), dma((GROUPS, 2)),
            dma((GROUPS, 2)), dma((GROUPS, 2)),
            dma((GROUPS, 2)), dma((GROUPS, 2)),
            dma((GROUPS, 2)), dma((GROUPS, 2)),
            dma((GROUPS, 2)), dma((GROUPS, 2)),
            dma((4,)), dma((4,)),
            dma((6,)), dma((6,)),
            dma((4,)), dma((4,)),
        ],
        compiler_params=pltpu.CompilerParams(
            collective_id=0, has_side_effects=True, vmem_limit_bytes=56 * 1024 * 1024
        ),
        name="sketch",
    )(codes, signs, slab)


def solution(mesh):
    return jax.shard_map(
        shards,
        mesh=mesh,
        in_specs=(P("rows", "cols"), P("rows"), P()),
        out_specs=P("rows", "cols"),
        check_vma=False,
    )
```

```python
import functools

import jax
import jax.numpy as jnp
from jax import lax
from jax.experimental import pallas as pl
from jax.experimental.pallas import tpu as pltpu
from jax.sharding import PartitionSpec as P

HEIGHT = 8192
SLOTS = 1024
GROUPS = 8
STEP = SLOTS // GROUPS
HALF = STEP // 2
WIDE = 128
MESH = pl.DeviceIdType.MESH
SCALE = 1.0 / (8 * SLOTS * 8 * HEIGHT)

ORDER = (
    (0, 0, 2), (0, 1, 2), (0, 0, 0), (0, 2, 2), (0, 0, 3), (1, 0, 0), (0, 0, 1), (1, 1, 0),
    (0, 1, 0), (1, 2, 0), (0, 3, 2), (2, 0, 0), (0, 1, 3), (2, 0, 1), (0, 1, 1), (0, 2, 0),
    (0, 4, 2), (1, 3, 0), (0, 2, 3), (2, 1, 0), (0, 2, 1), (3, 0, 0), (3, 0, 1), (2, 1, 1),
    (0, 3, 0), (1, 4, 0), (0, 5, 2), (3, 1, 0), (3, 1, 1), (2, 2, 0), (0, 3, 3), (2, 2, 1),
    (0, 3, 1), (3, 2, 0), (3, 2, 1), (0, 4, 0), (1, 5, 0), (0, 6, 2), (2, 3, 0), (0, 4, 3),
    (2, 3, 1), (0, 4, 1), (3, 3, 0), (3, 3, 1), (0, 5, 0), (1, 6, 0), (0, 7, 2), (2, 4, 0),
    (0, 5, 3), (2, 4, 1), (4, 0, 0), (0, 5, 1), (0, 6, 0), (1, 7, 0), (3, 4, 0), (3, 4, 1),
    (0, 6, 3), (2, 5, 0), (0, 6, 1), (4, 1, 0), (2, 5, 1), (0, 7, 0), (0, 7, 3), (2, 6, 0),
    (0, 7, 1), (4, 2, 0), (2, 6, 1), (3, 5, 0), (3, 5, 1), (2, 7, 0), (2, 7, 1), (5, 0, 0),
    (5, 0, 1), (5, 0, 2), (5, 0, 3), (4, 3, 0), (5, 1, 0), (5, 1, 1), (5, 1, 2), (5, 1, 3),
    (3, 6, 0), (3, 6, 1), (5, 2, 0), (5, 2, 1), (5, 2, 2), (5, 2, 3), (3, 7, 0), (3, 7, 1),
    (6, 0, 0), (4, 4, 0), (5, 3, 0), (5, 3, 1), (5, 3, 2), (5, 3, 3), (6, 1, 0), (4, 5, 0),
    (6, 2, 0), (4, 6, 0), (4, 7, 0), (5, 4, 0), (5, 4, 1), (5, 4, 2), (5, 4, 3), (6, 3, 0),
    (5, 5, 0), (5, 5, 1), (5, 5, 2), (5, 5, 3), (5, 6, 0), (5, 6, 1), (5, 6, 2), (5, 6, 3),
    (5, 7, 0), (5, 7, 1), (5, 7, 2), (5, 7, 3), (6, 4, 0), (6, 5, 0), (6, 6, 0), (6, 7, 0),
)


def parity_of(bits):
    bits = bits ^ (bits >> 4)
    bits = bits ^ (bits >> 2)
    bits = bits ^ (bits >> 1)
    return bits & 1


def split(value):
    high = value.astype(jnp.bfloat16)
    low = (value - high.astype(jnp.float32)).astype(jnp.bfloat16)
    return high, low


def kernel(
    samples, bits, slab, out,
    raw, table, matrix, code_rows, codes, mine, theirs, from_core, from_x1, from_x2, ybuf, zbuf,
    gram, core_gram, from_c1, from_c2, final, arrived,
    load_sem, code_sem, d_send, d_recv, x1_send, x1_recv, x2_send, x2_recv,
    y_send, y_recv, yf_send, yf_recv, z_send, z_recv, zf_send, zf_recv,
    c1_send, c1_recv, c2_send, c2_recv, c3_send, c3_recv, c4_send, c4_recv,
):
    row = lax.axis_index("rows")
    col = lax.axis_index("cols")
    x, k = row // 2, row % 2
    y, z = col // 4, col % 4
    partner = (row + 1 - 2 * k, col)
    x_sides = ((((x + 3) % 4) * 2 + k, col), (((x + 1) % 4) * 2 + k, col))
    y_sides = ((row, ((y + 3) % 4) * 4 + z), (row, ((y + 1) % 4) * 4 + z))
    z_sides = ((row, y * 4 + (z + 3) % 4), (row, y * 4 + (z + 1) % 4))
    owners = [(x * 2 + z // 2, y * 4 + 2 * k + j) for j in range(2)]

    loads = []
    for part in range(8):
        rows = pl.ds(part * 1024, 1024)
        loads.append(pltpu.make_async_copy(slab.at[rows], raw.at[rows], load_sem.at[part]))
        loads[-1].start()

    barrier = pltpu.get_barrier_semaphore()
    for other in (partner, *x_sides, *y_sides, *z_sides):
        pl.semaphore_signal(barrier, inc=1, device_id=other, device_id_type=MESH)
    for j in range(2):
        @pl.when(2 * k + j != z)
        def _():
            pl.semaphore_signal(barrier, inc=1, device_id=owners[j], device_id_type=MESH)

    code_rows[...] = samples[...] % HEIGHT + HEIGHT * parity_of((samples[...] // HEIGHT) & row)

    left = lax.broadcasted_iota(jnp.int32, (256, 256), 0)
    right = lax.broadcasted_iota(jnp.int32, (256, 256), 1)
    matrix[...] = (1 - 2 * parity_of(left & right)).astype(jnp.float32).astype(jnp.bfloat16)

    def inside(q):
        signs = [
            (1 - 2 * bits[pl.ds(2 * q + i, 1), :]).astype(jnp.float32).astype(jnp.bfloat16)
            for i in range(2)
        ]
        signed = matrix[...] * jnp.concatenate(signs, axis=1)
        start = pl.multiple_of(q * 256, 256)
        high, low = split(raw[pl.ds(start, 256), :])
        both = jnp.dot(
            signed, jnp.concatenate([high, low], axis=1), preferred_element_type=jnp.float32
        )
        table[pl.ds(start, 256), :] = both[:, :128] + both[:, 128:]

    def two_inside(i, carry):
        inside(2 * i)
        inside(2 * i + 1)
        return carry

    code_copy = pltpu.make_async_copy(code_rows, codes, code_sem)
    for part in range(8):
        loads[part].wait()
        lax.fori_loop(part * 2, part * 2 + 2, two_inside, 0)
        if part == 1:
            code_copy.start()

    def across(t, carry):
        starts = [pl.multiple_of(q * 256 + t * 8, 8) for q in range(32)]
        values = [table[pl.ds(start, 8), :] for start in starts]
        span = 1
        while span < 32:
            for base in range(0, 32, 2 * span):
                for i in range(base, base + span):
                    first, second = values[i], values[i + span]
                    values[i], values[i + span] = first + second, first - second
            span *= 2
        for start, value in zip(starts, values):
            table[pl.ds(start, 8), :] = value
            table[pl.ds(start + HEIGHT, 8), :] = -value
        return carry

    lax.fori_loop(0, 32, across, 0)
    code_copy.wait()

    pl.semaphore_wait(barrier, 8 + (z // 2 - k) * (z // 2 - k))

    def gather(g, d, core, target):
        base = (((x + d) % 4) * 2 + core) * SLOTS + g * STEP

        def eight(i, carry):
            at = base + i * 8
            to = pl.multiple_of(g * STEP + i * 8, 8)
            for u in range(8):
                target[d, pl.ds(to + u, 1), :] = table[pl.ds(codes[at + u], 1), :]
            return carry

        lax.fori_loop(0, STEP // 8, eight, 0)

    def remote(source, target, send, recv, device):
        return pltpu.make_async_remote_copy(
            src_ref=source, dst_ref=target, send_sem=send, recv_sem=recv,
            device_id=device, device_id_type=MESH,
        )

    sent = []

    def go(copy):
        copy.start()
        sent.append(copy)

    def slots(g):
        return pl.ds(g * STEP, STEP)

    def half(g, side):
        return pl.ds(g * STEP + side * HALF, HALF)

    distances = (3, 1)

    def core_copy(g, d):
        return remote(
            theirs.at[d, slots(g)], from_core.at[d, slots(g)],
            d_send.at[g, d], d_recv.at[g, d], partner,
        )

    def x1_copy(g, side):
        return remote(
            mine.at[2, half(g, side)], from_x1.at[side, pl.ds(g * HALF, HALF)],
            x1_send.at[g, side], x1_recv.at[g, side], x_sides[side],
        )

    def x2_copy(g, side, late):
        rows = half(g, side if late else 1 - side)
        return remote(
            mine.at[distances[side], rows], from_x2.at[side, rows],
            x2_send.at[g, side, late], x2_recv.at[g, side, late], x_sides[side],
        )

    def z_near(g, side, block):
        return remote(
            zbuf.at[block, slots(g)], zbuf.at[block, slots(g)],
            z_send.at[g, side], z_recv.at[g, side], z_sides[side],
        )

    def z_far(g, side, block):
        return remote(
            zbuf.at[block, half(g, side)], zbuf.at[block, half(g, side)],
            zf_send.at[g, side], zf_recv.at[g, side], z_sides[side],
        )

    def y_near(g, side, block):
        return remote(
            ybuf.at[g, block], ybuf.at[g, block],
            y_send.at[g, side], y_recv.at[g, side], y_sides[side],
        )

    def y_far(g, side, block):
        rows = pl.ds(64 * side, 64)
        return remote(
            ybuf.at[g, block, rows], ybuf.at[g, block, rows],
            yf_send.at[g, side], yf_recv.at[g, side], y_sides[side],
        )

    def came(at, side):
        return ((at + 1) % 4, (at + 3) % 4)[side]

    def take_rows(g, d):
        gather(g, d, 1 - k, theirs)
        go(core_copy(g, d))
        gather(g, d, k, mine)

    def send_x1(g, _):
        core_copy(g, 2).wait_recv()
        mine[2, slots(g)] = mine[2, slots(g)] + from_core[2, slots(g)]
        go(x1_copy(g, 0))
        go(x1_copy(g, 1))

    def send_x2_early(g, side):
        d = distances[side]
        core_copy(g, d).wait_recv()
        mine[d, slots(g)] = mine[d, slots(g)] + from_core[d, slots(g)]
        go(x2_copy(g, side, 0))

    def send_x2_late(g, side):
        d = distances[side]
        x1_copy(g, side).wait_recv()
        rows = half(g, side)
        mine[d, rows] = mine[d, rows] + from_x1[side, pl.ds(g * HALF, HALF)]
        go(x2_copy(g, side, 1))

    def send_yz(g, _):
        core_copy(g, 0).wait_recv()
        for side in range(2):
            for late in range(2):
                x2_copy(g, side, late).wait_recv()
        rows = slots(g)
        block = (mine[0, rows] + from_core[0, rows]) + (from_x2[0, rows] + from_x2[1, rows])
        zbuf[z, rows] = block
        ybuf[g, y] = block.T
        for side in range(2):
            go(z_near(g, side, z))
            go(y_near(g, side, y))

    def forward(g, which):
        side = which % 2
        if which < 2:
            y_near(g, side, came(y, side)).wait_recv()
            go(y_far(g, side, came(y, side)))
        else:
            z_near(g, side, came(z, side)).wait_recv()
            go(z_far(g, side, came(z, side)))

    def multiply(g, _):
        for side in range(2):
            y_far(g, side, (y + 2) % 4).wait_recv()
            z_far(g, side, (z + 2) % 4).wait_recv()
        right = []
        for h in range(2):
            high, low = split(
                jnp.concatenate([zbuf[2 * h, slots(g)], zbuf[2 * h + 1, slots(g)]], axis=1)
            )
            right.append(jnp.concatenate([high, low, high], axis=0))
        for m in range(2):
            high, low = split(
                jnp.concatenate([ybuf[g, 2 * m], ybuf[g, 2 * m + 1]], axis=0)
            )
            left = jnp.concatenate([high, high, low], axis=1)
            for h in range(2):
                value = jnp.dot(left, right[h], preferred_element_type=jnp.float32)
                for i in range(2):
                    part = value[i * 128:(i + 1) * 128]
                    if g:
                        part = part + gram[2 * m + i, h]
                    gram[2 * m + i, h] = part

    steps = (take_rows, send_x1, send_x2_early, send_x2_late, send_yz, forward, multiply)
    for kind, group, side in ORDER:
        steps[kind](group, side)

    def c1_copy(d):
        at = (x + d) % 4
        return remote(
            gram.at[at, 1 - k], core_gram.at[at], c1_send.at[d], c1_recv.at[d], partner
        )

    def combine(d):
        at = (x + d) % 4
        c1_copy(d).wait_recv()
        core_gram[at] = core_gram[at] + gram[at, k]

    def c2_copy(side):
        return remote(
            core_gram.at[(x + 2) % 4, pl.ds(64 * side, 64)], from_c1.at[side],
            c2_send.at[side], c2_recv.at[side], x_sides[side],
        )

    def c3_copy(side, late):
        rows = pl.ds(64 * (side if late else 1 - side), 64)
        return remote(
            core_gram.at[(x + distances[side]) % 4, rows], from_c2.at[side, rows],
            c3_send.at[side, late], c3_recv.at[side, late], x_sides[side],
        )

    for d in (2, 3, 1, 0):
        go(c1_copy(d))
    combine(2)
    for side in range(2):
        go(c2_copy(side))
    for side in range(2):
        combine(distances[side])
        go(c3_copy(side, 0))
    combine(0)
    for side in range(2):
        c2_copy(side).wait_recv()
        at = (x + distances[side]) % 4
        rows = pl.ds(64 * side, 64)
        core_gram[at, rows] = core_gram[at, rows] + from_c1[side]
        go(c3_copy(side, 1))
    for side in range(2):
        for late in range(2):
            c3_copy(side, late).wait_recv()
    total = (core_gram[x] + (from_c2[0] + from_c2[1])) * SCALE

    def c4_copy(j, slot):
        return remote(
            final.at[j], arrived.at[slot], c4_send.at[j], c4_recv.at[slot], owners[j]
        )

    for j in range(2):
        final[j] = total[:, j * 128:(j + 1) * 128]
    for j in range(2):
        @pl.when(2 * k + j != z)
        def _():
            c4_copy(j, z % 2).start()

        @pl.when(2 * k + j == z)
        def _():
            out[pl.ds(j * 128, 128), :] = total[:, j * 128:(j + 1) * 128]

    for copy in sent:
        copy.wait_send()
    for j in range(2):
        @pl.when(2 * k + j != z)
        def _():
            c4_copy(j, j).wait_recv()
            out[pl.ds(j * 128, 128), :] = arrived[j]
            c4_copy(j, j).wait_send()


def shards(slab, sign_bits, sample_rows):
    dma = pltpu.SemaphoreType.DMA
    vmem = lambda *shape: pltpu.VMEM(shape, jnp.float32)
    pairs = [dma((GROUPS, 2))] * 2
    return pl.pallas_call(
        kernel,
        out_shape=jax.ShapeDtypeStruct((256, 128), jnp.float32),
        in_specs=[
            pl.BlockSpec(memory_space=pltpu.VMEM),
            pl.BlockSpec(memory_space=pltpu.VMEM),
            pl.BlockSpec(memory_space=pl.ANY),
        ],
        out_specs=pl.BlockSpec(memory_space=pltpu.VMEM),
        scratch_shapes=[
            vmem(HEIGHT, WIDE),
            vmem(2 * HEIGHT, WIDE),
            pltpu.VMEM((256, 256), jnp.bfloat16),
            pltpu.VMEM((8 * SLOTS,), jnp.int32),
            pltpu.SMEM((8 * SLOTS,), jnp.int32),
            vmem(4, SLOTS, WIDE),
            vmem(4, SLOTS, WIDE),
            vmem(4, SLOTS, WIDE),
            vmem(2, SLOTS // 2, WIDE),
            vmem(2, SLOTS, WIDE),
            vmem(GROUPS, 4, WIDE, STEP),
            vmem(4, SLOTS, WIDE),
            vmem(4, 2, 128, 256),
            vmem(4, 128, 256),
            vmem(2, 64, 256),
            vmem(2, 128, 256),
            vmem(2, 128, 128),
            vmem(2, 128, 128),
            dma((8,)), dma(()),
            dma((GROUPS, 4)), dma((GROUPS, 4)),
            *pairs,
            dma((GROUPS, 2, 2)), dma((GROUPS, 2, 2)),
            *pairs, *pairs, *pairs, *pairs,
            dma((4,)), dma((4,)),
            dma((2,)), dma((2,)),
            dma((2, 2)), dma((2, 2)),
            dma((2,)), dma((2,)),
        ],
        compiler_params=pltpu.CompilerParams(
            collective_id=0, has_side_effects=True, vmem_limit_bytes=56 * 1024 * 1024
        ),
        name="sketch",
    )(sample_rows, sign_bits.reshape(64, 128), slab)


def solution(mesh):
    return jax.shard_map(
        shards,
        mesh=mesh,
        in_specs=(P("rows", "cols"), P("rows"), P()),
        out_specs=P("rows", "cols"),
        check_vma=False,
    )
```

```python
import functools

import jax
import jax.numpy as jnp
from jax import lax
from jax.experimental import pallas as pl
from jax.experimental.pallas import tpu as pltpu
from jax.sharding import PartitionSpec as P

HEIGHT = 8192
SLOTS = 1024
GROUPS = 8
STEP = SLOTS // GROUPS
HALF = STEP // 2
PITCH = 264
NEGATED = HEIGHT // 256 * PITCH
WIDE = 128
MESH = pl.DeviceIdType.MESH
SCALE = 1.0 / (8 * SLOTS * 8 * HEIGHT)

ORDER = (
    (0, 0, 2), (0, 1, 2), (0, 0, 0), (0, 2, 2), (0, 1, 0), (0, 3, 2), (1, 0, 0), (0, 0, 1),
    (1, 1, 0), (0, 0, 3), (1, 2, 0), (0, 2, 0), (0, 4, 2), (1, 3, 0), (0, 1, 1), (2, 0, 1),
    (0, 1, 3), (2, 0, 0), (0, 3, 0), (0, 5, 2), (1, 4, 0), (0, 2, 1), (2, 1, 1), (0, 2, 3),
    (2, 1, 0), (0, 4, 0), (3, 0, 0), (0, 6, 2), (1, 5, 0), (0, 3, 1), (3, 1, 0), (2, 2, 1),
    (0, 3, 3), (2, 2, 0), (0, 5, 0), (3, 2, 0), (0, 7, 2), (1, 6, 0), (0, 4, 1), (2, 3, 1),
    (0, 4, 3), (2, 3, 0), (3, 3, 0), (0, 6, 0), (0, 5, 1), (1, 7, 0), (0, 5, 3), (2, 4, 1),
    (0, 7, 0), (2, 4, 0), (3, 4, 0), (0, 6, 1), (0, 6, 3), (2, 5, 1), (0, 7, 1), (2, 5, 0),
    (0, 7, 3), (4, 0, 0), (2, 6, 1), (2, 6, 0), (3, 5, 0), (2, 7, 1), (2, 7, 0), (4, 1, 0),
    (4, 2, 0), (3, 6, 0), (5, 0, 0), (5, 0, 1), (4, 3, 0), (5, 1, 0), (5, 1, 1), (3, 7, 0),
    (5, 2, 0), (5, 2, 1), (4, 4, 0), (5, 3, 0), (5, 3, 1), (4, 5, 0), (6, 1, 1), (4, 6, 0),
    (4, 7, 0), (5, 4, 0), (5, 4, 1), (6, 3, 1), (5, 5, 0), (5, 5, 1), (5, 6, 0), (5, 6, 1),
    (5, 7, 0), (5, 7, 1), (6, 5, 1), (6, 6, 0), (6, 7, 0),
)


def parity_of(bits):
    bits = bits ^ (bits >> 4)
    bits = bits ^ (bits >> 2)
    bits = bits ^ (bits >> 1)
    return bits & 1


def split(value):
    high = value.astype(jnp.bfloat16)
    low = (value - high.astype(jnp.float32)).astype(jnp.bfloat16)
    return high, low


def kernel(
    samples_in, bits_in, slab, out,
    samples, bits, raw, table, matrix, code_rows, codes, mine, theirs, from_core, from_x1, from_x2,
    ybuf, zbuf, gram, core_gram, from_c1, from_c2, final,
    load_sem, code_sem, d_recv, x1_recv, x2_recv, y_recv, z_recv, far_recv,
    c1_recv, c2_recv, c3_recv, c4_recv, c4_send,
    d_send, x1_send, x2_send, near_send, far_send, c1_send, c2_send, c3_send,
):
    row = lax.axis_index("rows")
    col = lax.axis_index("cols")
    x, k = row // 2, row % 2
    y, z = col // 4, col % 4
    partner = (row + 1 - 2 * k, col)
    x_sides = ((((x + 3) % 4) * 2 + k, col), (((x + 1) % 4) * 2 + k, col))
    y_sides = ((row, ((y + 3) % 4) * 4 + z), (row, ((y + 1) % 4) * 4 + z))
    z_sides = ((row, y * 4 + (z + 3) % 4), (row, y * 4 + (z + 1) % 4))
    owners = [(x * 2 + z // 2, y * 4 + 2 * k + j) for j in range(2)]

    loads = [
        pltpu.make_async_copy(bits_in, bits, load_sem.at[8]),
        pltpu.make_async_copy(samples_in, samples, load_sem.at[9]),
    ]
    for part in range(8):
        rows = pl.ds(part * 1024, 1024)
        loads.append(pltpu.make_async_copy(slab.at[rows], raw.at[rows], load_sem.at[part]))
    for load in (loads[0], loads[2], loads[1], *loads[3:]):
        load.start()

    barrier = pltpu.get_barrier_semaphore()
    for other in (partner, *x_sides, *y_sides, *z_sides):
        pl.semaphore_signal(barrier, inc=1, device_id=other, device_id_type=MESH)
    for j in range(2):
        @pl.when(2 * k + j != z)
        def _():
            pl.semaphore_signal(barrier, inc=1, device_id=owners[j], device_id_type=MESH)

    left = lax.broadcasted_iota(jnp.int32, (256, 256), 0)
    right = lax.broadcasted_iota(jnp.int32, (256, 256), 1)
    matrix[...] = (1 - 2 * parity_of(left & right)).astype(jnp.float32).astype(jnp.bfloat16)

    def inside(q):
        signs = [
            (1 - 2 * bits[pl.ds(2 * q + i, 1), :]).astype(jnp.float32).astype(jnp.bfloat16)
            for i in range(2)
        ]
        signed = matrix[...] * jnp.concatenate(signs, axis=1)
        start = pl.multiple_of(q * 256, 256)
        high, low = split(raw[pl.ds(start, 256), :])
        both = jnp.dot(
            signed, jnp.concatenate([high, low], axis=1), preferred_element_type=jnp.float32
        )
        table[pl.ds(pl.multiple_of(q * PITCH, 8), 256), :] = both[:, :128] + both[:, 128:]

    def four_inside(i, carry):
        for u in range(4):
            inside(4 * i + u)
        return carry

    code_copy = pltpu.make_async_copy(code_rows, codes, code_sem)
    loads[0].wait()
    for part in range(8):
        loads[2 + part].wait()
        four_inside(part, 0)
        if part == 1:
            loads[1].wait()
            parity = parity_of((samples[...] // HEIGHT) & row)
            offset = samples[...] % HEIGHT
            code_rows[...] = offset + offset // 256 * (PITCH - 256) + NEGATED * parity
        if part == 3:
            code_copy.start()

    def across(t, carry):
        starts = [pl.multiple_of(q * PITCH + t * 8, 8) for q in range(32)]
        values = [table[pl.ds(start, 8), :] for start in starts]
        span = 1
        while span < 32:
            for base in range(0, 32, 2 * span):
                for i in range(base, base + span):
                    first, second = values[i], values[i + span]
                    values[i], values[i + span] = first + second, first - second
            span *= 2
        for start, value in zip(starts, values):
            table[pl.ds(start, 8), :] = value
            table[pl.ds(start + NEGATED, 8), :] = -value
        return carry

    lax.fori_loop(0, 32, across, 0)
    code_copy.wait()

    pl.semaphore_wait(barrier, 8 + (z // 2 - k) * (z // 2 - k))

    def gather(g, d, core, target):
        base = (((x + d) % 4) * 2 + core) * SLOTS + g * STEP

        def some(i, carry):
            at = base + i * 32
            to = pl.multiple_of(g * STEP + i * 32, 32)
            for u in range(32):
                target[d, pl.ds(to + u, 1), :] = table[pl.ds(codes[at + u], 1), :]
            return carry

        lax.fori_loop(0, STEP // 32, some, 0)

    def remote(source, target, send, recv, device):
        return pltpu.make_async_remote_copy(
            src_ref=source, dst_ref=target, send_sem=send, recv_sem=recv,
            device_id=device, device_id_type=MESH,
        )

    def slots(g):
        return pl.ds(g * STEP, STEP)

    def half(g, side):
        return pl.ds(g * STEP + side * HALF, HALF)

    distances = (3, 1)

    def core_copy(g, d):
        return remote(
            theirs.at[d, slots(g)], from_core.at[d, slots(g)], d_send, d_recv.at[g, d], partner
        )

    def x1_copy(g, side):
        rows = half(g, side)
        return remote(mine.at[2, rows], from_x1.at[rows], x1_send, x1_recv.at[g], x_sides[side])

    def x2_copy(g, side, late):
        part = side if late else 1 - side
        return remote(
            mine.at[distances[side], half(g, part)], from_x2.at[g, side, pl.ds(part * HALF, HALF)],
            x2_send, x2_recv.at[g], x_sides[side],
        )

    def z_near(g, side):
        own = zbuf.at[z, slots(g)]
        return remote(own, own, near_send, z_recv.at[g], z_sides[side])

    def y_near(g, side):
        own = ybuf.at[g, y]
        return remote(own, own, near_send, y_recv.at[g], y_sides[side])

    def came(at, side):
        return ((at + 1) % 4, (at + 3) % 4)[side]

    def z_far(g, side):
        part = zbuf.at[came(z, side), half(g, side)]
        return remote(part, part, far_send, far_recv.at[g], z_sides[side])

    def y_far(g, side):
        part = ybuf.at[g, came(y, side), pl.ds(64 * side, 64)]
        return remote(part, part, far_send, far_recv.at[g], y_sides[side])

    def arrived(like, semaphore):
        remote(like, like, semaphore, semaphore, partner).wait_recv()

    def left_here(like, semaphore):
        remote(like, like, semaphore, semaphore, partner).wait_send()

    def take_rows(g, d):
        gather(g, d, 1 - k, theirs)
        core_copy(g, d).start()
        gather(g, d, k, mine)

    def send_x1(g, _):
        core_copy(g, 2).wait_recv()
        mine[2, slots(g)] = mine[2, slots(g)] + from_core[2, slots(g)]
        x1_copy(g, 0).start()
        x1_copy(g, 1).start()

    def send_x2_early(g, side):
        d = distances[side]
        core_copy(g, d).wait_recv()
        mine[d, slots(g)] = mine[d, slots(g)] + from_core[d, slots(g)]
        x2_copy(g, side, 0).start()

    def send_x2_late(g, _):
        arrived(from_x1.at[slots(g)], x1_recv.at[g])
        for side in range(2):
            d, rows = distances[side], half(g, side)
            mine[d, rows] = mine[d, rows] + from_x1[rows]
            x2_copy(g, side, 1).start()

    def send_yz(g, _):
        core_copy(g, 0).wait_recv()
        arrived(from_x2.at[g], x2_recv.at[g])
        rows = slots(g)
        block = (mine[0, rows] + from_core[0, rows]) + (from_x2[g, 0] + from_x2[g, 1])
        zbuf[z, rows] = block
        ybuf[g, y] = block.T
        for side in range(2):
            z_near(g, side).start()
            y_near(g, side).start()

    def forward(g, which):
        arrived(from_x2.at[g], (y_recv, z_recv)[which].at[g])
        for side in range(2):
            (y_far, z_far)[which](g, side).start()

    def multiply(g, more):
        groups = (g,) if not more else (g - 1, g)
        for each in groups:
            arrived(from_x2.at[each], far_recv.at[each])
        rows = pl.ds(groups[0] * STEP, STEP * len(groups))
        right = []
        for h in range(2):
            high, low = split(
                jnp.concatenate([zbuf[2 * h, rows], zbuf[2 * h + 1, rows]], axis=1)
            )
            right.append(jnp.concatenate([high, low, high], axis=0))
        for m in range(2):
            high, low = split(
                jnp.concatenate(
                    [
                        jnp.concatenate([ybuf[each, 2 * m], ybuf[each, 2 * m + 1]], axis=0)
                        for each in groups
                    ],
                    axis=1,
                )
            )
            left = jnp.concatenate([high, high, low], axis=1)
            for h in range(2):
                value = jnp.dot(left, right[h], preferred_element_type=jnp.float32)
                for i in range(2):
                    part = value[i * 128:(i + 1) * 128]
                    if groups[0]:
                        part = part + gram[2 * m + i, h]
                    gram[2 * m + i, h] = part

    steps = (take_rows, send_x1, send_x2_early, send_x2_late, send_yz, forward, multiply)
    for kind, group, side in ORDER:
        steps[kind](group, side)

    def c1_copy(d):
        at = (x + d) % 4
        return remote(gram.at[at, 1 - k], core_gram.at[at], c1_send, c1_recv.at[d], partner)

    def combine(d):
        at = (x + d) % 4
        c1_copy(d).wait_recv()
        core_gram[at] = core_gram[at] + gram[at, k]

    def c2_copy(side):
        rows = pl.ds(64 * side, 64)
        return remote(
            core_gram.at[(x + 2) % 4, rows], from_c1.at[rows], c2_send, c2_recv, x_sides[side]
        )

    def c3_copy(side, late):
        rows = pl.ds(64 * (side if late else 1 - side), 64)
        return remote(
            core_gram.at[(x + distances[side]) % 4, rows], from_c2.at[side, rows],
            c3_send, c3_recv, x_sides[side],
        )

    for d in (2, 3, 1, 0):
        c1_copy(d).start()
    combine(2)
    for side in range(2):
        c2_copy(side).start()
    for side in range(2):
        combine(distances[side])
        c3_copy(side, 0).start()
    combine(0)
    arrived(from_c1, c2_recv)
    for side in range(2):
        at = (x + distances[side]) % 4
        rows = pl.ds(64 * side, 64)
        core_gram[at, rows] = core_gram[at, rows] + from_c1[rows]
        c3_copy(side, 1).start()
    left_here(theirs, d_send)
    left_here(mine.at[2], x1_send)
    left_here(from_x2, x2_send)
    left_here(theirs, near_send)
    left_here(from_x2, far_send)
    arrived(from_c2, c3_recv)
    total = (core_gram[x] + (from_c2[0] + from_c2[1])) * SCALE

    def c4_copy(j, slot):
        return remote(
            final.at[j], out.at[pl.ds(pl.multiple_of(slot * 128, 128), 128)],
            c4_send.at[j], c4_recv.at[slot], owners[j],
        )

    def own_copy(j):
        return pltpu.make_async_copy(final.at[j], out.at[pl.ds(j * 128, 128)], c4_send.at[j])

    for j in range(2):
        final[j] = total[:, j * 128:(j + 1) * 128]
    for j in range(2):
        @pl.when(2 * k + j != z)
        def _():
            c4_copy(j, z % 2).start()

        @pl.when(2 * k + j == z)
        def _():
            own_copy(j).start()

    left_here(core_gram, c1_send)
    left_here(from_c1, c2_send)
    left_here(from_c2, c3_send)
    for j in range(2):
        @pl.when(2 * k + j != z)
        def _():
            c4_copy(j, j).wait()

        @pl.when(2 * k + j == z)
        def _():
            own_copy(j).wait()


def shards(slab, sign_bits, sample_rows):
    dma = pltpu.SemaphoreType.DMA
    vmem = lambda *shape: pltpu.VMEM(shape, jnp.float32)
    return pl.pallas_call(
        kernel,
        out_shape=jax.ShapeDtypeStruct((256, 128), jnp.float32),
        in_specs=[
            pl.BlockSpec(memory_space=pltpu.HBM),
            pl.BlockSpec(memory_space=pltpu.HBM),
            pl.BlockSpec(memory_space=pltpu.HBM),
        ],
        out_specs=pl.BlockSpec(memory_space=pltpu.HBM),
        scratch_shapes=[
            pltpu.VMEM((8 * SLOTS,), jnp.int32),
            pltpu.VMEM((HEIGHT // WIDE, WIDE), jnp.int32),
            vmem(HEIGHT, WIDE),
            vmem(2 * NEGATED, WIDE),
            pltpu.VMEM((256, 256), jnp.bfloat16),
            pltpu.VMEM((8 * SLOTS,), jnp.int32),
            pltpu.SMEM((8 * SLOTS,), jnp.int32),
            vmem(4, SLOTS, WIDE),
            vmem(4, SLOTS, WIDE),
            vmem(4, SLOTS, WIDE),
            vmem(SLOTS, WIDE),
            vmem(GROUPS, 2, STEP, WIDE),
            vmem(GROUPS, 4, WIDE, STEP),
            vmem(4, SLOTS, WIDE),
            vmem(4, 2, 128, 256),
            vmem(4, 128, 256),
            vmem(128, 256),
            vmem(2, 128, 256),
            vmem(2, 128, 128),
            dma((10,)), dma(()), dma((GROUPS, 4)),
            *[dma((GROUPS,))] * 5,
            dma((4,)), dma(()), dma(()), dma((2,)), dma((2,)),
            *[dma(())] * 8,
        ],
        compiler_params=pltpu.CompilerParams(
            collective_id=0, has_side_effects=True, vmem_limit_bytes=56 * 1024 * 1024
        ),
        name="sketch",
    )(sample_rows, sign_bits.reshape(64, 128), slab)


def solution(mesh):
    return jax.shard_map(
        shards,
        mesh=mesh,
        in_specs=(P("rows", "cols"), P("rows"), P()),
        out_specs=P("rows", "cols"),
        check_vma=False,
    )
```

```python
import functools

import jax
import jax.numpy as jnp
from jax import lax
from jax.experimental import pallas as pl
from jax.experimental.pallas import tpu as pltpu
from jax.sharding import PartitionSpec as P

HEIGHT = 8192
SLOTS = 1024
GROUPS = 8
STEP = SLOTS // GROUPS
HALF = STEP // 2
PITCH = 264
NEGATED = HEIGHT // 256 * PITCH
WIDE = 128
MESH = pl.DeviceIdType.MESH
SCALE = 1.0 / (8 * SLOTS * 8 * HEIGHT)

ORDER = (
    (0, 0, 2), (0, 1, 2), (0, 2, 1), (0, 2, 2), (0, 0, 1), (1, 0, 0), (0, 0, 3), (1, 1, 0),
    (0, 3, 2), (0, 5, 2), (1, 2, 0), (0, 3, 3), (0, 1, 3), (1, 3, 0), (2, 2, 1), (2, 0, 1),
    (0, 0, 0), (0, 4, 3), (2, 0, 0), (2, 3, 0), (0, 3, 1), (0, 1, 1), (0, 4, 2), (3, 0, 0),
    (0, 6, 3), (2, 1, 0), (2, 1, 1), (3, 1, 0), (2, 3, 1), (0, 2, 3), (0, 7, 1), (0, 5, 3),
    (0, 2, 0), (0, 4, 0), (0, 6, 2), (2, 2, 0), (3, 2, 0), (0, 3, 0), (0, 1, 0), (1, 4, 0),
    (0, 7, 3), (0, 6, 1), (4, 0, 0), (3, 3, 0), (0, 5, 1), (0, 7, 2), (1, 5, 0), (2, 4, 0),
    (0, 4, 1), (4, 1, 0), (1, 7, 0), (1, 6, 0), (2, 4, 1), (4, 2, 0), (3, 4, 0), (2, 5, 0),
    (4, 3, 0), (2, 5, 1), (5, 1, 0), (2, 7, 0), (2, 7, 1), (5, 0, 1), (3, 5, 0), (2, 6, 0),
    (5, 1, 1), (2, 6, 1), (5, 0, 0), (5, 2, 1), (5, 2, 0), (0, 6, 0), (3, 6, 0), (4, 4, 0),
    (5, 3, 1), (3, 7, 0), (5, 3, 0), (0, 5, 0), (0, 7, 0), (4, 5, 0), (4, 6, 0), (4, 7, 0),
    (6, 1, 1), (5, 5, 1), (5, 4, 0), (5, 5, 0), (5, 4, 1), (5, 6, 1), (5, 6, 0), (5, 7, 1),
    (5, 7, 0), (6, 3, 1), (6, 5, 1), (6, 6, 0), (6, 7, 0),
)


def parity_of(bits):
    bits = bits ^ (bits >> 4)
    bits = bits ^ (bits >> 2)
    bits = bits ^ (bits >> 1)
    return bits & 1


def split(value):
    high = value.astype(jnp.bfloat16)
    low = (value - high.astype(jnp.float32)).astype(jnp.bfloat16)
    return high, low


def kernel(
    samples_in, bits_in, slab, out,
    samples, bits, raw, table, matrix, code_rows, codes, mine, theirs, from_core, from_x1, from_x2,
    ybuf, zbuf, gram, core_gram, from_c1, from_c2, final,
    load_sem, code_sem, d_recv, x1_recv, x2_recv, y_recv, z_recv, far_recv,
    c1_recv, c2_recv, c3_recv, c4_recv, c4_send,
    d_send, x1_send, x2_send, near_send, far_send, c1_send, c2_send, c3_send,
):
    row = lax.axis_index("rows")
    col = lax.axis_index("cols")
    x, k = row // 2, row % 2
    y, z = col // 4, col % 4
    partner = (row + 1 - 2 * k, col)
    x_sides = ((((x + 3) % 4) * 2 + k, col), (((x + 1) % 4) * 2 + k, col))
    y_sides = ((row, ((y + 3) % 4) * 4 + z), (row, ((y + 1) % 4) * 4 + z))
    z_sides = ((row, y * 4 + (z + 3) % 4), (row, y * 4 + (z + 1) % 4))
    owners = [(x * 2 + z // 2, y * 4 + 2 * k + j) for j in range(2)]

    loads = [
        pltpu.make_async_copy(bits_in, bits, load_sem.at[8]),
        pltpu.make_async_copy(samples_in, samples, load_sem.at[9]),
    ]
    for part in range(8):
        rows = pl.ds(part * 1024, 1024)
        loads.append(pltpu.make_async_copy(slab.at[rows], raw.at[rows], load_sem.at[part]))
    for load in (loads[0], loads[2], loads[1], *loads[3:]):
        load.start()

    barrier = pltpu.get_barrier_semaphore()
    for other in (partner, *x_sides, *y_sides, *z_sides):
        pl.semaphore_signal(barrier, inc=1, device_id=other, device_id_type=MESH)
    for j in range(2):
        @pl.when(2 * k + j != z)
        def _():
            pl.semaphore_signal(barrier, inc=1, device_id=owners[j], device_id_type=MESH)

    left = lax.broadcasted_iota(jnp.int32, (256, 256), 0)
    right = lax.broadcasted_iota(jnp.int32, (256, 256), 1)
    matrix[...] = (1 - 2 * parity_of(left & right)).astype(jnp.float32).astype(jnp.bfloat16)

    def inside(q):
        signs = [
            (1 - 2 * bits[pl.ds(2 * q + i, 1), :]).astype(jnp.float32).astype(jnp.bfloat16)
            for i in range(2)
        ]
        signed = matrix[...] * jnp.concatenate(signs, axis=1)
        start = pl.multiple_of(q * 256, 256)
        high, low = split(raw[pl.ds(start, 256), :])
        both = jnp.dot(
            signed, jnp.concatenate([high, low], axis=1), preferred_element_type=jnp.float32
        )
        table[pl.ds(pl.multiple_of(q * PITCH, 8), 256), :] = both[:, :128] + both[:, 128:]

    def four_inside(i, carry):
        for u in range(4):
            inside(4 * i + u)
        return carry

    code_copy = pltpu.make_async_copy(code_rows, codes, code_sem)
    loads[0].wait()
    for part in range(8):
        loads[2 + part].wait()
        four_inside(part, 0)
        if part == 1:
            loads[1].wait()
            parity = parity_of((samples[...] // HEIGHT) & row)
            offset = samples[...] % HEIGHT
            code_rows[...] = offset + offset // 256 * (PITCH - 256) + NEGATED * parity
        if part == 3:
            code_copy.start()

    def across(t, carry):
        starts = [pl.multiple_of(q * PITCH + t * 8, 8) for q in range(32)]
        values = [table[pl.ds(start, 8), :] for start in starts]
        span = 1
        while span < 32:
            for base in range(0, 32, 2 * span):
                for i in range(base, base + span):
                    first, second = values[i], values[i + span]
                    values[i], values[i + span] = first + second, first - second
            span *= 2
        for start, value in zip(starts, values):
            table[pl.ds(start, 8), :] = value
            table[pl.ds(start + NEGATED, 8), :] = -value
        return carry

    lax.fori_loop(0, 32, across, 0)
    code_copy.wait()

    pl.semaphore_wait(barrier, 8 + (z // 2 - k) * (z // 2 - k))

    def gather(g, d, core, target):
        base = (((x + d) % 4) * 2 + core) * SLOTS + g * STEP

        def some(i, carry):
            at = base + i * 32
            to = pl.multiple_of(g * STEP + i * 32, 32)
            for u in range(32):
                target[d, pl.ds(to + u, 1), :] = table[pl.ds(codes[at + u], 1), :]
            return carry

        lax.fori_loop(0, STEP // 32, some, 0)

    def remote(source, target, send, recv, device):
        return pltpu.make_async_remote_copy(
            src_ref=source, dst_ref=target, send_sem=send, recv_sem=recv,
            device_id=device, device_id_type=MESH,
        )

    def slots(g):
        return pl.ds(g * STEP, STEP)

    def half(g, side):
        return pl.ds(g * STEP + side * HALF, HALF)

    distances = (3, 1)

    def core_copy(g, d):
        return remote(
            theirs.at[d, slots(g)], from_core.at[d, slots(g)], d_send, d_recv.at[g, d], partner
        )

    def x1_copy(g, side):
        rows = half(g, side)
        return remote(mine.at[2, rows], from_x1.at[rows], x1_send, x1_recv.at[g], x_sides[side])

    def x2_copy(g, side, late):
        part = side if late else 1 - side
        return remote(
            mine.at[distances[side], half(g, part)], from_x2.at[g, side, pl.ds(part * HALF, HALF)],
            x2_send, x2_recv.at[g], x_sides[side],
        )

    def z_near(g, side, part):
        own = zbuf.at[z, half(g, side if part == 0 else 1 - side)]
        return remote(own, own, near_send, (z_recv, far_recv)[part].at[g], z_sides[side])

    def y_near(g, side, part):
        own = ybuf.at[g, y, pl.ds(64 * (side if part == 0 else 1 - side), 64)]
        return remote(own, own, near_send, (y_recv, far_recv)[part].at[g], y_sides[side])

    def came(at, side):
        return ((at + 1) % 4, (at + 3) % 4)[side]

    def z_far(g, side):
        part = zbuf.at[came(z, side), half(g, side)]
        return remote(part, part, far_send, far_recv.at[g], z_sides[side])

    def y_far(g, side):
        part = ybuf.at[g, came(y, side), pl.ds(64 * side, 64)]
        return remote(part, part, far_send, far_recv.at[g], y_sides[side])

    def arrived(like, semaphore):
        remote(like, like, semaphore, semaphore, partner).wait_recv()

    def left_here(like, semaphore):
        remote(like, like, semaphore, semaphore, partner).wait_send()

    def take_rows(g, d):
        gather(g, d, 1 - k, theirs)
        core_copy(g, d).start()
        gather(g, d, k, mine)

    def send_x1(g, _):
        core_copy(g, 2).wait_recv()
        mine[2, slots(g)] = mine[2, slots(g)] + from_core[2, slots(g)]
        x1_copy(g, 0).start()
        x1_copy(g, 1).start()

    def send_x2_early(g, side):
        d = distances[side]
        core_copy(g, d).wait_recv()
        mine[d, slots(g)] = mine[d, slots(g)] + from_core[d, slots(g)]
        x2_copy(g, side, 0).start()

    def send_x2_late(g, _):
        arrived(from_x1.at[slots(g)], x1_recv.at[g])
        for side in range(2):
            d, rows = distances[side], half(g, side)
            mine[d, rows] = mine[d, rows] + from_x1[rows]
            x2_copy(g, side, 1).start()

    def send_yz(g, _):
        core_copy(g, 0).wait_recv()
        arrived(from_x2.at[g], x2_recv.at[g])
        rows = slots(g)
        block = (mine[0, rows] + from_core[0, rows]) + (from_x2[g, 0] + from_x2[g, 1])
        zbuf[z, rows] = block
        ybuf[g, y] = block.T
        for part in range(2):
            for side in range(2):
                z_near(g, side, part).start()
                y_near(g, side, part).start()

    def forward(g, which):
        arrived(from_x1.at[slots(g)], (y_recv, z_recv)[which].at[g])
        for side in range(2):
            (y_far, z_far)[which](g, side).start()

    def multiply(g, more):
        groups = (g,) if not more else (g - 1, g)
        for each in groups:
            arrived(from_x2.at[pl.ds(0, 2)], far_recv.at[each])
        rows = pl.ds(groups[0] * STEP, STEP * len(groups))
        right = []
        for h in range(2):
            high, low = split(
                jnp.concatenate([zbuf[2 * h, rows], zbuf[2 * h + 1, rows]], axis=1)
            )
            right.append(jnp.concatenate([high, low, high], axis=0))
        for m in range(2):
            high, low = split(
                jnp.concatenate(
                    [
                        jnp.concatenate([ybuf[each, 2 * m], ybuf[each, 2 * m + 1]], axis=0)
                        for each in groups
                    ],
                    axis=1,
                )
            )
            left = jnp.concatenate([high, high, low], axis=1)
            for h in range(2):
                value = jnp.dot(left, right[h], preferred_element_type=jnp.float32)
                for i in range(2):
                    part = value[i * 128:(i + 1) * 128]
                    if groups[0]:
                        part = part + gram[2 * m + i, h]
                    gram[2 * m + i, h] = part

    def c1_copy(d):
        at = (x + d) % 4
        return remote(gram.at[at, 1 - k], core_gram.at[at], c1_send, c1_recv.at[d], partner)

    def multiply_last(g):
        arrived(from_x2.at[pl.ds(0, 2)], far_recv.at[g])
        right = []
        for h in range(2):
            high, low = split(
                jnp.concatenate([zbuf[2 * h, slots(g)], zbuf[2 * h + 1, slots(g)]], axis=1)
            )
            right.append(jnp.concatenate([high, low, high], axis=0))
        for d in (2, 3, 1, 0):
            at = (x + d) % 4
            high, low = split(ybuf[g, at])
            left = jnp.concatenate([high, high, low], axis=1)
            for h in range(2):
                gram[at, h] = gram[at, h] + jnp.dot(
                    left, right[h], preferred_element_type=jnp.float32
                )
            c1_copy(d).start()

    steps = (take_rows, send_x1, send_x2_early, send_x2_late, send_yz, forward, multiply)
    for kind, group, side in ORDER[:-1]:
        steps[kind](group, side)
    multiply_last(GROUPS - 1)

    def combine(d):
        at = (x + d) % 4
        c1_copy(d).wait_recv()
        core_gram[at] = core_gram[at] + gram[at, k]

    def c_rows(side, part):
        return pl.ds(64 * part + 32 * side, 32)

    def c2_copy(side, part):
        rows = c_rows(side, part)
        return remote(
            core_gram.at[(x + 2) % 4, rows], from_c1.at[rows], c2_send, c2_recv.at[part],
            x_sides[side],
        )

    def c3_copy(side, part, late):
        rows = c_rows(side if late else 1 - side, part)
        return remote(
            core_gram.at[(x + distances[side]) % 4, rows], from_c2.at[side, rows],
            c3_send, c3_recv.at[part if late else 0], x_sides[side],
        )

    def c4_copy(j, slot, part):
        rows = pl.ds(64 * part, 64)
        return remote(
            final.at[j, rows], out.at[pl.ds(pl.multiple_of(slot * 128 + 64 * part, 64), 64)],
            c4_send.at[j], c4_recv.at[slot], owners[j],
        )

    def c4_both(j):
        return remote(
            final.at[j], out.at[pl.ds(j * 128, 128)], c4_send.at[j], c4_recv.at[j], owners[j]
        )

    def own_copy(j):
        return pltpu.make_async_copy(final.at[j], out.at[pl.ds(j * 128, 128)], c4_send.at[j])

    combine(2)
    for part in range(2):
        for side in range(2):
            c2_copy(side, part).start()
    for side in range(2):
        combine(distances[side])
        for part in range(2):
            c3_copy(side, part, 0).start()
    combine(0)
    for part in range(2):
        arrived(from_c1.at[pl.ds(0, 64)], c2_recv.at[part])
        for side in range(2):
            at, rows = (x + distances[side]) % 4, c_rows(side, part)
            core_gram[at, rows] = core_gram[at, rows] + from_c1[rows]
            c3_copy(side, part, 1).start()
    left_here(theirs, d_send)
    left_here(mine.at[2], x1_send)
    left_here(from_x2, x2_send)
    left_here(theirs, near_send)
    left_here(from_x2, far_send)
    for part in range(2):
        like = core_gram.at[0, pl.ds(0, 64)] if part else core_gram.at[pl.ds(0, 3), pl.ds(0, 64)]
        arrived(like, c3_recv.at[part])
        rows = pl.ds(64 * part, 64)
        total = (core_gram[x, rows] + (from_c2[0, rows] + from_c2[1, rows])) * SCALE
        for j in range(2):
            final[j, rows] = total[:, j * 128:(j + 1) * 128]
        for j in range(2):
            @pl.when(2 * k + j != z)
            def _():
                c4_copy(j, z % 2, part).start()

            if part:
                @pl.when(2 * k + j == z)
                def _():
                    own_copy(j).start()

    left_here(core_gram, c1_send)
    left_here(from_c1, c2_send)
    left_here(from_c2, c3_send)
    for j in range(2):
        @pl.when(2 * k + j != z)
        def _():
            c4_both(j).wait()

        @pl.when(2 * k + j == z)
        def _():
            own_copy(j).wait()


def shards(slab, sign_bits, sample_rows):
    dma = pltpu.SemaphoreType.DMA
    vmem = lambda *shape: pltpu.VMEM(shape, jnp.float32)
    return pl.pallas_call(
        kernel,
        out_shape=jax.ShapeDtypeStruct((256, 128), jnp.float32),
        in_specs=[
            pl.BlockSpec(memory_space=pltpu.HBM),
            pl.BlockSpec(memory_space=pltpu.HBM),
            pl.BlockSpec(memory_space=pltpu.HBM),
        ],
        out_specs=pl.BlockSpec(memory_space=pltpu.HBM),
        scratch_shapes=[
            pltpu.VMEM((8 * SLOTS,), jnp.int32),
            pltpu.VMEM((HEIGHT // WIDE, WIDE), jnp.int32),
            vmem(HEIGHT, WIDE),
            vmem(2 * NEGATED, WIDE),
            pltpu.VMEM((256, 256), jnp.bfloat16),
            pltpu.VMEM((8 * SLOTS,), jnp.int32),
            pltpu.SMEM((8 * SLOTS,), jnp.int32),
            vmem(4, SLOTS, WIDE),
            vmem(4, SLOTS, WIDE),
            vmem(4, SLOTS, WIDE),
            vmem(SLOTS, WIDE),
            vmem(GROUPS, 2, STEP, WIDE),
            vmem(GROUPS, 4, WIDE, STEP),
            vmem(4, SLOTS, WIDE),
            vmem(4, 2, 128, 256),
            vmem(4, 128, 256),
            vmem(128, 256),
            vmem(2, 128, 256),
            vmem(2, 128, 128),
            dma((10,)), dma(()), dma((GROUPS, 4)),
            *[dma((GROUPS,))] * 5,
            dma((4,)), dma((2,)), dma((2,)), dma((2,)), dma((2,)),
            *[dma(())] * 8,
        ],
        compiler_params=pltpu.CompilerParams(
            collective_id=0, has_side_effects=True, vmem_limit_bytes=56 * 1024 * 1024
        ),
        name="sketch",
    )(sample_rows, sign_bits.reshape(64, 128), slab)


def solution(mesh):
    return jax.shard_map(
        shards,
        mesh=mesh,
        in_specs=(P("rows", "cols"), P("rows"), P()),
        out_specs=P("rows", "cols"),
        check_vma=False,
    )
```

```python
import functools

import jax
import jax.numpy as jnp
from jax import lax
from jax.experimental import pallas as pl
from jax.experimental.pallas import tpu as pltpu
from jax.sharding import PartitionSpec as P

HEIGHT = 8192
SLOTS = 1024
GROUPS = 8
STEP = SLOTS // GROUPS
HALF = STEP // 2
PITCH = 264
NEGATED = HEIGHT // 256 * PITCH
WIDE = 128
MESH = pl.DeviceIdType.MESH
SCALE = 1.0 / (8 * SLOTS * 8 * HEIGHT)

ORDER = (
    (0, 0, 2), (0, 1, 2), (0, 0, 1), (0, 2, 2), (0, 1, 1), (1, 0, 0), (0, 0, 3), (1, 1, 0),
    (0, 3, 2), (0, 4, 2), (1, 2, 0), (0, 1, 3), (0, 2, 3), (1, 3, 0), (2, 0, 0), (2, 0, 1),
    (0, 0, 0), (0, 3, 3), (2, 1, 0), (2, 1, 1), (0, 2, 1), (0, 3, 1), (0, 5, 2), (3, 0, 0),
    (0, 4, 3), (2, 2, 0), (2, 2, 1), (3, 1, 0), (2, 3, 0), (0, 5, 3), (0, 4, 1), (0, 6, 3),
    (0, 1, 0), (0, 2, 0), (0, 6, 2), (2, 3, 1), (3, 2, 0), (0, 3, 0), (0, 4, 0), (1, 4, 0),
    (0, 7, 3), (0, 5, 1), (4, 0, 0), (3, 3, 0), (0, 6, 1), (0, 7, 2), (1, 5, 0), (2, 4, 0),
    (0, 7, 1), (4, 1, 0), (1, 6, 0), (1, 7, 0), (2, 4, 1), (4, 2, 0), (3, 4, 0), (2, 5, 0),
    (4, 3, 0), (2, 5, 1), (5, 0, 0), (2, 6, 0), (2, 6, 1), (5, 0, 1), (3, 5, 0), (2, 7, 0),
    (5, 1, 0), (2, 7, 1), (5, 1, 1), (5, 2, 0), (5, 2, 1), (0, 5, 0), (3, 6, 0), (4, 4, 0),
    (5, 3, 0), (3, 7, 0), (5, 3, 1), (0, 6, 0), (0, 7, 0), (4, 5, 0), (4, 6, 0), (4, 7, 0),
    (6, 1, 1), (5, 4, 0), (5, 4, 1), (5, 5, 0), (5, 5, 1), (5, 6, 0), (5, 6, 1), (5, 7, 0),
    (5, 7, 1), (6, 3, 1), (6, 5, 1), (6, 6, 0), (6, 7, 0),
)


def parity_of(bits):
    bits = bits ^ (bits >> 4)
    bits = bits ^ (bits >> 2)
    bits = bits ^ (bits >> 1)
    return bits & 1


def split(value):
    high = value.astype(jnp.bfloat16)
    low = (value - high.astype(jnp.float32)).astype(jnp.bfloat16)
    return high, low


def kernel(
    samples_in, bits_in, slab, out,
    samples, bits, raw, table, matrix, code_rows, codes, mine, theirs, from_core, from_x1, from_x2,
    ybuf, zbuf, gram, core_gram, from_c1, from_c2, final,
    load_sem, code_sem, d_recv, x1_recv, x2_recv, y_recv, z_recv, far_recv,
    c1_recv, c2_recv, c3_recv, c4_recv, c4_send,
    d_send, x1_send, x2_send, near_send, far_send, c1_send, c2_send, c3_send,
):
    row = lax.axis_index("rows")
    col = lax.axis_index("cols")
    x, k = row // 2, row % 2
    y, z = col // 4, col % 4
    partner = (row + 1 - 2 * k, col)
    x_sides = ((((x + 3) % 4) * 2 + k, col), (((x + 1) % 4) * 2 + k, col))
    y_sides = ((row, ((y + 3) % 4) * 4 + z), (row, ((y + 1) % 4) * 4 + z))
    z_sides = ((row, y * 4 + (z + 3) % 4), (row, y * 4 + (z + 1) % 4))
    owners = [(x * 2 + z // 2, y * 4 + 2 * k + j) for j in range(2)]

    loads = [
        pltpu.make_async_copy(bits_in, bits, load_sem.at[8]),
        pltpu.make_async_copy(samples_in, samples, load_sem.at[9]),
    ]
    for part in range(8):
        rows = pl.ds(part * 1024, 1024)
        loads.append(pltpu.make_async_copy(slab.at[rows], raw.at[rows], load_sem.at[part]))
    for load in (loads[0], loads[2], loads[1], *loads[3:]):
        load.start()

    barrier = pltpu.get_barrier_semaphore()
    for other in (partner, *x_sides, *y_sides, *z_sides):
        pl.semaphore_signal(barrier, inc=1, device_id=other, device_id_type=MESH)
    for j in range(2):
        @pl.when(2 * k + j != z)
        def _():
            pl.semaphore_signal(barrier, inc=1, device_id=owners[j], device_id_type=MESH)

    left = lax.broadcasted_iota(jnp.int32, (256, 256), 0)
    right = lax.broadcasted_iota(jnp.int32, (256, 256), 1)
    matrix[...] = (1 - 2 * parity_of(left & right)).astype(jnp.float32).astype(jnp.bfloat16)

    def inside(q):
        signs = [
            (1 - 2 * bits[pl.ds(2 * q + i, 1), :]).astype(jnp.float32).astype(jnp.bfloat16)
            for i in range(2)
        ]
        signed = matrix[...] * jnp.concatenate(signs, axis=1)
        start = q * 256
        high, low = split(raw[pl.ds(start, 256), :])
        both = jnp.dot(
            signed, jnp.concatenate([high, low], axis=1), preferred_element_type=jnp.float32
        )
        table[pl.ds(q * PITCH, 256), :] = both[:, :128] + both[:, 128:]

    code_copy = pltpu.make_async_copy(code_rows, codes, code_sem)
    loads[0].wait()
    ends = (1, 4, 8)
    for last, end in enumerate(ends):
        for part in range(0 if last == 0 else ends[last - 1], end):
            loads[2 + part].wait()
        for q in range(0 if last == 0 else 4 * ends[last - 1], 4 * end):
            inside(q)
        if last == 0:
            loads[1].wait()
            parity = parity_of((samples[...] // HEIGHT) & row)
            offset = samples[...] % HEIGHT
            code_rows[...] = offset + offset // 256 * (PITCH - 256) + NEGATED * parity
        if last == 1:
            code_copy.start()

    def across(t, carry):
        starts = [pl.multiple_of(q * PITCH + t * 8, 8) for q in range(32)]
        values = [table[pl.ds(start, 8), :] for start in starts]
        span = 1
        while span < 32:
            for base in range(0, 32, 2 * span):
                for i in range(base, base + span):
                    first, second = values[i], values[i + span]
                    values[i], values[i + span] = first + second, first - second
            span *= 2
        for start, value in zip(starts, values):
            table[pl.ds(start, 8), :] = value
            table[pl.ds(start + NEGATED, 8), :] = -value
        return carry

    lax.fori_loop(0, 32, across, 0)
    code_copy.wait()

    pl.semaphore_wait(barrier, 8 + (z // 2 - k) * (z // 2 - k))

    def gather(g, d, core, target):
        base = (((x + d) % 4) * 2 + core) * SLOTS + g * STEP

        def some(i, carry):
            at = base + i * 32
            to = pl.multiple_of(g * STEP + i * 32, 32)
            for u in range(32):
                target[d, pl.ds(to + u, 1), :] = table[pl.ds(codes[at + u], 1), :]
            return carry

        lax.fori_loop(0, STEP // 32, some, 0)

    def remote(source, target, send, recv, device):
        return pltpu.make_async_remote_copy(
            src_ref=source, dst_ref=target, send_sem=send, recv_sem=recv,
            device_id=device, device_id_type=MESH,
        )

    def slots(g):
        return pl.ds(g * STEP, STEP)

    def half(g, side):
        return pl.ds(g * STEP + side * HALF, HALF)

    distances = (3, 1)

    def core_copy(g, d):
        return remote(
            theirs.at[d, slots(g)], from_core.at[d, slots(g)], d_send, d_recv.at[g, d], partner
        )

    def x1_copy(g, side):
        rows = half(g, side)
        return remote(mine.at[2, rows], from_x1.at[rows], x1_send, x1_recv.at[g], x_sides[side])

    def x2_copy(g, side, late):
        part = side if late else 1 - side
        return remote(
            mine.at[distances[side], half(g, part)], from_x2.at[g, side, pl.ds(part * HALF, HALF)],
            x2_send, x2_recv.at[g], x_sides[side],
        )

    def z_near(g, side, part):
        own = zbuf.at[z, half(g, side if part == 0 else 1 - side)]
        return remote(own, own, near_send, (z_recv, far_recv)[part].at[g], z_sides[side])

    def y_near(g, side, part):
        own = ybuf.at[g, y, pl.ds(64 * (side if part == 0 else 1 - side), 64)]
        return remote(own, own, near_send, (y_recv, far_recv)[part].at[g], y_sides[side])

    def came(at, side):
        return ((at + 1) % 4, (at + 3) % 4)[side]

    def z_far(g, side):
        part = zbuf.at[came(z, side), half(g, side)]
        return remote(part, part, far_send, far_recv.at[g], z_sides[side])

    def y_far(g, side):
        part = ybuf.at[g, came(y, side), pl.ds(64 * side, 64)]
        return remote(part, part, far_send, far_recv.at[g], y_sides[side])

    def arrived(like, semaphore):
        remote(like, like, semaphore, semaphore, partner).wait_recv()

    def left_here(like, semaphore):
        remote(like, like, semaphore, semaphore, partner).wait_send()

    def take_rows(g, d):
        gather(g, d, 1 - k, theirs)
        core_copy(g, d).start()
        gather(g, d, k, mine)

    def send_x1(g, _):
        core_copy(g, 2).wait_recv()
        mine[2, slots(g)] = mine[2, slots(g)] + from_core[2, slots(g)]
        x1_copy(g, 0).start()
        x1_copy(g, 1).start()

    def send_x2_early(g, side):
        d = distances[side]
        core_copy(g, d).wait_recv()
        mine[d, slots(g)] = mine[d, slots(g)] + from_core[d, slots(g)]
        x2_copy(g, side, 0).start()

    def send_x2_late(g, _):
        arrived(from_x1.at[slots(g)], x1_recv.at[g])
        for side in range(2):
            d, rows = distances[side], half(g, side)
            mine[d, rows] = mine[d, rows] + from_x1[rows]
            x2_copy(g, side, 1).start()

    def send_yz(g, _):
        core_copy(g, 0).wait_recv()
        arrived(from_x2.at[g], x2_recv.at[g])
        rows = slots(g)
        block = (mine[0, rows] + from_core[0, rows]) + (from_x2[g, 0] + from_x2[g, 1])
        zbuf[z, rows] = block
        ybuf[g, y] = block.T
        for part in range(2):
            for side in range(2):
                z_near(g, side, part).start()
                y_near(g, side, part).start()

    def forward(g, which):
        arrived(from_x1.at[slots(g)], (y_recv, z_recv)[which].at[g])
        for side in range(2):
            (y_far, z_far)[which](g, side).start()

    def multiply(g, more):
        groups = (g,) if not more else (g - 1, g)
        for each in groups:
            arrived(from_x2.at[pl.ds(0, 2)], far_recv.at[each])
        rows = pl.ds(groups[0] * STEP, STEP * len(groups))
        right = []
        for h in range(2):
            high, low = split(
                jnp.concatenate([zbuf[2 * h, rows], zbuf[2 * h + 1, rows]], axis=1)
            )
            right.append(jnp.concatenate([high, low, high], axis=0))
        for m in range(2):
            high, low = split(
                jnp.concatenate(
                    [
                        jnp.concatenate([ybuf[each, 2 * m], ybuf[each, 2 * m + 1]], axis=0)
                        for each in groups
                    ],
                    axis=1,
                )
            )
            left = jnp.concatenate([high, high, low], axis=1)
            for h in range(2):
                value = jnp.dot(left, right[h], preferred_element_type=jnp.float32)
                for i in range(2):
                    part = value[i * 128:(i + 1) * 128]
                    if groups[0]:
                        part = part + gram[2 * m + i, h]
                    gram[2 * m + i, h] = part

    def c1_copy(d):
        at = (x + d) % 4
        return remote(gram.at[at, 1 - k], core_gram.at[at], c1_send, c1_recv.at[d], partner)

    def multiply_last(g):
        arrived(from_x2.at[pl.ds(0, 2)], far_recv.at[g])
        right = []
        for h in range(2):
            high, low = split(
                jnp.concatenate([zbuf[2 * h, slots(g)], zbuf[2 * h + 1, slots(g)]], axis=1)
            )
            right.append(jnp.concatenate([high, low, high], axis=0))
        for d in (2, 3, 1, 0):
            at = (x + d) % 4
            high, low = split(ybuf[g, at])
            left = jnp.concatenate([high, high, low], axis=1)
            for h in range(2):
                gram[at, h] = gram[at, h] + jnp.dot(
                    left, right[h], preferred_element_type=jnp.float32
                )
            c1_copy(d).start()

    steps = (take_rows, send_x1, send_x2_early, send_x2_late, send_yz, forward, multiply)
    for kind, group, side in ORDER[:-1]:
        steps[kind](group, side)
    multiply_last(GROUPS - 1)

    def combine(d):
        at = (x + d) % 4
        c1_copy(d).wait_recv()
        core_gram[at] = core_gram[at] + gram[at, k]

    def c_rows(side, part):
        return pl.ds(64 * part + 32 * side, 32)

    def c2_copy(side, part):
        rows = c_rows(side, part)
        return remote(
            core_gram.at[(x + 2) % 4, rows], from_c1.at[rows], c2_send, c2_recv.at[part],
            x_sides[side],
        )

    def c3_copy(side, part, late):
        rows = c_rows(side if late else 1 - side, part)
        return remote(
            core_gram.at[(x + distances[side]) % 4, rows], from_c2.at[side, rows],
            c3_send, c3_recv.at[part if late else 0], x_sides[side],
        )

    def c4_copy(j, slot, part):
        rows = pl.ds(64 * part, 64)
        return remote(
            final.at[j, rows], out.at[pl.ds(pl.multiple_of(slot * 128 + 64 * part, 64), 64)],
            c4_send.at[j], c4_recv.at[slot], owners[j],
        )

    def c4_both(j):
        return remote(
            final.at[j], out.at[pl.ds(j * 128, 128)], c4_send.at[j], c4_recv.at[j], owners[j]
        )

    def own_copy(j):
        return pltpu.make_async_copy(final.at[j], out.at[pl.ds(j * 128, 128)], c4_send.at[j])

    combine(2)
    for part in range(2):
        for side in range(2):
            c2_copy(side, part).start()
    for side in range(2):
        combine(distances[side])
        for part in range(2):
            c3_copy(side, part, 0).start()
    combine(0)
    for part in range(2):
        arrived(from_c1.at[pl.ds(0, 64)], c2_recv.at[part])
        for side in range(2):
            at, rows = (x + distances[side]) % 4, c_rows(side, part)
            core_gram[at, rows] = core_gram[at, rows] + from_c1[rows]
            c3_copy(side, part, 1).start()
    left_here(theirs, d_send)
    left_here(mine.at[2], x1_send)
    left_here(from_x2, x2_send)
    left_here(theirs, near_send)
    left_here(from_x2, far_send)
    for part in range(2):
        like = core_gram.at[0, pl.ds(0, 64)] if part else core_gram.at[pl.ds(0, 3), pl.ds(0, 64)]
        arrived(like, c3_recv.at[part])
        rows = pl.ds(64 * part, 64)
        total = (core_gram[x, rows] + (from_c2[0, rows] + from_c2[1, rows])) * SCALE
        for j in range(2):
            final[j, rows] = total[:, j * 128:(j + 1) * 128]
        for j in range(2):
            @pl.when(2 * k + j != z)
            def _():
                c4_copy(j, z % 2, part).start()

            if part:
                @pl.when(2 * k + j == z)
                def _():
                    own_copy(j).start()

    left_here(core_gram, c1_send)
    left_here(from_c1, c2_send)
    left_here(from_c2, c3_send)
    for j in range(2):
        @pl.when(2 * k + j != z)
        def _():
            c4_both(j).wait()

        @pl.when(2 * k + j == z)
        def _():
            own_copy(j).wait()


def shards(slab, sign_bits, sample_rows):
    dma = pltpu.SemaphoreType.DMA
    vmem = lambda *shape: pltpu.VMEM(shape, jnp.float32)
    return pl.pallas_call(
        kernel,
        out_shape=jax.ShapeDtypeStruct((256, 128), jnp.float32),
        in_specs=[
            pl.BlockSpec(memory_space=pltpu.HBM),
            pl.BlockSpec(memory_space=pltpu.HBM),
            pl.BlockSpec(memory_space=pltpu.HBM),
        ],
        out_specs=pl.BlockSpec(memory_space=pltpu.HBM),
        scratch_shapes=[
            pltpu.VMEM((8 * SLOTS,), jnp.int32),
            pltpu.VMEM((HEIGHT // WIDE, WIDE), jnp.int32),
            vmem(HEIGHT, WIDE),
            vmem(2 * NEGATED, WIDE),
            pltpu.VMEM((256, 256), jnp.bfloat16),
            pltpu.VMEM((8 * SLOTS,), jnp.int32),
            pltpu.SMEM((8 * SLOTS,), jnp.int32),
            vmem(4, SLOTS, WIDE),
            vmem(4, SLOTS, WIDE),
            vmem(4, SLOTS, WIDE),
            vmem(SLOTS, WIDE),
            vmem(GROUPS, 2, STEP, WIDE),
            vmem(GROUPS, 4, WIDE, STEP),
            vmem(4, SLOTS, WIDE),
            vmem(4, 2, 128, 256),
            vmem(4, 128, 256),
            vmem(128, 256),
            vmem(2, 128, 256),
            vmem(2, 128, 128),
            dma((10,)), dma(()), dma((GROUPS, 4)),
            *[dma((GROUPS,))] * 5,
            dma((4,)), dma((2,)), dma((2,)), dma((2,)), dma((2,)),
            *[dma(())] * 8,
        ],
        compiler_params=pltpu.CompilerParams(
            collective_id=0, has_side_effects=True, vmem_limit_bytes=56 * 1024 * 1024
        ),
        name="sketch",
    )(sample_rows, sign_bits.reshape(64, 128), slab)


def solution(mesh):
    return jax.shard_map(
        shards,
        mesh=mesh,
        in_specs=(P("rows", "cols"), P("rows"), P()),
        out_specs=P("rows", "cols"),
        check_vma=False,
    )
```

```python
import functools

import jax
import jax.numpy as jnp
from jax import lax
from jax.experimental import pallas as pl
from jax.experimental.pallas import tpu as pltpu
from jax.sharding import PartitionSpec as P

HEIGHT = 8192
SLOTS = 1024
GROUPS = 8
STEP = SLOTS // GROUPS
HALF = STEP // 2
PARTS = 4
PITCH = 264
NEGATED = HEIGHT // 256 * PITCH
WIDE = 128
MESH = pl.DeviceIdType.MESH
SCALE = 1.0 / (8 * SLOTS * 8 * HEIGHT)

ORDER = (
    (0, 0, 2), (0, 0, 1), (0, 1, 2), (0, 2, 2), (0, 0, 3), (1, 0, 0), (0, 3, 2), (1, 1, 0),
    (0, 4, 2), (1, 2, 0), (0, 1, 1), (0, 1, 3), (2, 0, 0), (1, 3, 0), (0, 2, 1), (0, 5, 2),
    (0, 3, 1), (0, 2, 3), (2, 0, 1), (0, 4, 1), (0, 6, 2), (1, 4, 0), (3, 0, 0), (0, 0, 0),
    (0, 3, 3), (2, 1, 0), (2, 1, 1), (0, 5, 1), (0, 6, 1), (0, 4, 3), (0, 1, 0), (3, 1, 0),
    (2, 2, 0), (0, 7, 2), (0, 2, 0), (2, 2, 1), (0, 3, 0), (3, 2, 0), (2, 3, 0), (2, 3, 1),
    (0, 5, 3), (0, 4, 0), (3, 3, 0), (4, 0, 0), (1, 5, 0), (0, 5, 0), (0, 6, 3), (0, 7, 1),
    (4, 1, 0), (1, 6, 0), (0, 6, 0), (2, 4, 0), (2, 4, 1), (3, 4, 0), (1, 7, 0), (4, 2, 0),
    (2, 5, 0), (4, 3, 0), (0, 7, 3), (2, 5, 1), (5, 0, 0), (3, 5, 0), (2, 6, 0), (5, 0, 1),
    (2, 6, 1), (3, 6, 0), (2, 7, 0), (2, 7, 1), (5, 1, 0), (5, 1, 1), (5, 2, 0), (5, 2, 1),
    (4, 4, 0), (0, 7, 0), (3, 7, 0), (5, 3, 0), (5, 3, 1), (4, 5, 0), (4, 6, 0), (4, 7, 0),
    (6, 1, 1), (5, 4, 0), (5, 4, 1), (5, 5, 0), (5, 5, 1), (5, 6, 0), (5, 6, 1), (5, 7, 0),
    (5, 7, 1), (6, 3, 1), (6, 5, 1), (6, 6, 0), (6, 7, 0),
)


def parity_of(bits):
    bits = bits ^ (bits >> 4)
    bits = bits ^ (bits >> 2)
    bits = bits ^ (bits >> 1)
    return bits & 1


def split(value):
    high = value.astype(jnp.bfloat16)
    low = (value - high.astype(jnp.float32)).astype(jnp.bfloat16)
    return high, low


def kernel(
    samples_in, bits_in, slab, out,
    samples, bits, raw, table, matrix, code_rows, codes, mine, theirs, from_core, from_x1, from_x2,
    ybuf, zbuf, gram, core_gram, from_c1, from_c2, final,
    load_sem, code_sem, d_recv, x1_recv, x2_recv, y_recv, z_recv, far_recv,
    c1_recv, c2_recv, c3_recv, c4_recv, c4_send,
    d_send, x1_send, x2_send, near_send, far_send, c1_send, c2_send, c3_send,
):
    row = lax.axis_index("rows")
    col = lax.axis_index("cols")
    x, k = row // 2, row % 2
    y, z = col // 4, col % 4
    partner = (row + 1 - 2 * k, col)
    x_sides = ((((x + 3) % 4) * 2 + k, col), (((x + 1) % 4) * 2 + k, col))
    y_sides = ((row, ((y + 3) % 4) * 4 + z), (row, ((y + 1) % 4) * 4 + z))
    z_sides = ((row, y * 4 + (z + 3) % 4), (row, y * 4 + (z + 1) % 4))
    owners = [(x * 2 + z // 2, y * 4 + 2 * k + j) for j in range(2)]

    loads = [
        pltpu.make_async_copy(bits_in, bits, load_sem.at[8]),
        pltpu.make_async_copy(samples_in, samples, load_sem.at[9]),
    ]
    for part in range(8):
        rows = pl.ds(part * 1024, 1024)
        loads.append(pltpu.make_async_copy(slab.at[rows], raw.at[rows], load_sem.at[part]))
    for load in (loads[0], loads[2], loads[1], *loads[3:]):
        load.start()

    barrier = pltpu.get_barrier_semaphore()
    for other in (partner, *x_sides, *y_sides, *z_sides):
        pl.semaphore_signal(barrier, inc=1, device_id=other, device_id_type=MESH)
    for j in range(2):
        @pl.when(2 * k + j != z)
        def _():
            pl.semaphore_signal(barrier, inc=1, device_id=owners[j], device_id_type=MESH)

    left = lax.broadcasted_iota(jnp.int32, (256, 256), 0)
    right = lax.broadcasted_iota(jnp.int32, (256, 256), 1)
    matrix[...] = (1 - 2 * parity_of(left & right)).astype(jnp.float32).astype(jnp.bfloat16)

    def inside(q):
        signs = [
            (1 - 2 * bits[pl.ds(2 * q + i, 1), :]).astype(jnp.float32).astype(jnp.bfloat16)
            for i in range(2)
        ]
        signed = matrix[...] * jnp.concatenate(signs, axis=1)
        start = q * 256
        high, low = split(raw[pl.ds(start, 256), :])
        both = jnp.dot(
            signed, jnp.concatenate([high, low], axis=1), preferred_element_type=jnp.float32
        )
        table[pl.ds(q * PITCH, 256), :] = both[:, :128] + both[:, 128:]

    code_copy = pltpu.make_async_copy(code_rows, codes, code_sem)
    loads[0].wait()
    ends = (1, 4, 8)
    for last, end in enumerate(ends):
        for part in range(0 if last == 0 else ends[last - 1], end):
            loads[2 + part].wait()
        for q in range(0 if last == 0 else 4 * ends[last - 1], 4 * end):
            inside(q)
        if last == 0:
            loads[1].wait()
            parity = parity_of((samples[...] // HEIGHT) & row)
            offset = samples[...] % HEIGHT
            code_rows[...] = offset + offset // 256 * (PITCH - 256) + NEGATED * parity
        if last == 1:
            code_copy.start()

    def across(t, carry):
        starts = [pl.multiple_of(q * PITCH + t * 8, 8) for q in range(32)]
        values = [table[pl.ds(start, 8), :] for start in starts]
        span = 1
        while span < 32:
            for base in range(0, 32, 2 * span):
                for i in range(base, base + span):
                    first, second = values[i], values[i + span]
                    values[i], values[i + span] = first + second, first - second
            span *= 2
        for start, value in zip(starts, values):
            table[pl.ds(start, 8), :] = value
            table[pl.ds(start + NEGATED, 8), :] = -value
        return carry

    lax.fori_loop(0, 32, across, 0)
    code_copy.wait()

    pl.semaphore_wait(barrier, 8 + (z // 2 - k) * (z // 2 - k))

    def gather(g, d, core, target):
        base = (((x + d) % 4) * 2 + core) * SLOTS + g * STEP

        def some(i, carry):
            at = base + i * 32
            to = pl.multiple_of(g * STEP + i * 32, 32)
            for u in range(32):
                target[d, pl.ds(to + u, 1), :] = table[pl.ds(codes[at + u], 1), :]
            return carry

        lax.fori_loop(0, STEP // 32, some, 0)

    def remote(source, target, send, recv, device):
        return pltpu.make_async_remote_copy(
            src_ref=source, dst_ref=target, send_sem=send, recv_sem=recv,
            device_id=device, device_id_type=MESH,
        )

    def slots(g):
        return pl.ds(g * STEP, STEP)

    def half(g, side):
        return pl.ds(g * STEP + side * HALF, HALF)

    distances = (3, 1)

    def core_copy(g, d):
        return remote(
            theirs.at[d, slots(g)], from_core.at[d, slots(g)], d_send, d_recv.at[g, d], partner
        )

    def x1_copy(g, side):
        rows = half(g, side)
        return remote(mine.at[2, rows], from_x1.at[rows], x1_send, x1_recv.at[g], x_sides[side])

    def x2_copy(g, side, late):
        part = side if late else 1 - side
        return remote(
            mine.at[distances[side], half(g, part)], from_x2.at[g, side, pl.ds(part * HALF, HALF)],
            x2_send, x2_recv.at[g], x_sides[side],
        )

    def z_near(g, side, part):
        own = zbuf.at[z, half(g, side if part == 0 else 1 - side)]
        return remote(own, own, near_send, (z_recv, far_recv)[part].at[g], z_sides[side])

    def y_near(g, side, part):
        own = ybuf.at[g, y, pl.ds(64 * (side if part == 0 else 1 - side), 64)]
        return remote(own, own, near_send, (y_recv, far_recv)[part].at[g], y_sides[side])

    def came(at, side):
        return ((at + 1) % 4, (at + 3) % 4)[side]

    def z_far(g, side):
        part = zbuf.at[came(z, side), half(g, side)]
        return remote(part, part, far_send, far_recv.at[g], z_sides[side])

    def y_far(g, side):
        part = ybuf.at[g, came(y, side), pl.ds(64 * side, 64)]
        return remote(part, part, far_send, far_recv.at[g], y_sides[side])

    def arrived(like, semaphore):
        remote(like, like, semaphore, semaphore, partner).wait_recv()

    def left_here(like, semaphore):
        remote(like, like, semaphore, semaphore, partner).wait_send()

    def take_rows(g, d):
        gather(g, d, 1 - k, theirs)
        core_copy(g, d).start()
        gather(g, d, k, mine)

    def send_x1(g, _):
        core_copy(g, 2).wait_recv()
        mine[2, slots(g)] = mine[2, slots(g)] + from_core[2, slots(g)]
        x1_copy(g, 0).start()
        x1_copy(g, 1).start()

    def send_x2_early(g, side):
        d = distances[side]
        core_copy(g, d).wait_recv()
        mine[d, slots(g)] = mine[d, slots(g)] + from_core[d, slots(g)]
        x2_copy(g, side, 0).start()

    def send_x2_late(g, _):
        arrived(from_x1.at[slots(g)], x1_recv.at[g])
        for side in range(2):
            d, rows = distances[side], half(g, side)
            mine[d, rows] = mine[d, rows] + from_x1[rows]
            x2_copy(g, side, 1).start()

    def send_yz(g, _):
        core_copy(g, 0).wait_recv()
        arrived(from_x2.at[g], x2_recv.at[g])
        rows = slots(g)
        block = (mine[0, rows] + from_core[0, rows]) + (from_x2[g, 0] + from_x2[g, 1])
        zbuf[z, rows] = block
        ybuf[g, y] = block.T
        for part in range(2):
            for side in range(2):
                z_near(g, side, part).start()
                y_near(g, side, part).start()

    def forward(g, which):
        arrived(from_x1.at[slots(g)], (y_recv, z_recv)[which].at[g])
        for side in range(2):
            (y_far, z_far)[which](g, side).start()

    def multiply(g, more):
        groups = (g,) if not more else (g - 1, g)
        for each in groups:
            arrived(from_x2.at[pl.ds(0, 2)], far_recv.at[each])
        rows = pl.ds(groups[0] * STEP, STEP * len(groups))
        right = []
        for h in range(2):
            high, low = split(
                jnp.concatenate([zbuf[2 * h, rows], zbuf[2 * h + 1, rows]], axis=1)
            )
            right.append(jnp.concatenate([high, low, high], axis=0))
        for m in range(2):
            high, low = split(
                jnp.concatenate(
                    [
                        jnp.concatenate([ybuf[each, 2 * m], ybuf[each, 2 * m + 1]], axis=0)
                        for each in groups
                    ],
                    axis=1,
                )
            )
            left = jnp.concatenate([high, high, low], axis=1)
            for h in range(2):
                value = jnp.dot(left, right[h], preferred_element_type=jnp.float32)
                for i in range(2):
                    part = value[i * 128:(i + 1) * 128]
                    if groups[0]:
                        part = part + gram[2 * m + i, h]
                    gram[2 * m + i, h] = part

    def c1_copy(d):
        at = (x + d) % 4
        return remote(gram.at[at, 1 - k], core_gram.at[at], c1_send, c1_recv.at[d], partner)

    def multiply_last(g):
        arrived(from_x2.at[pl.ds(0, 2)], far_recv.at[g])
        right = []
        for h in range(2):
            high, low = split(
                jnp.concatenate([zbuf[2 * h, slots(g)], zbuf[2 * h + 1, slots(g)]], axis=1)
            )
            right.append(jnp.concatenate([high, low, high], axis=0))
        for d in (2, 3, 1, 0):
            at = (x + d) % 4
            high, low = split(ybuf[g, at])
            left = jnp.concatenate([high, high, low], axis=1)
            for h in range(2):
                gram[at, h] = gram[at, h] + jnp.dot(
                    left, right[h], preferred_element_type=jnp.float32
                )
            c1_copy(d).start()

    steps = (take_rows, send_x1, send_x2_early, send_x2_late, send_yz, forward, multiply)
    for kind, group, side in ORDER[:-1]:
        steps[kind](group, side)
    multiply_last(GROUPS - 1)

    def combine(d):
        at = (x + d) % 4
        c1_copy(d).wait_recv()
        core_gram[at] = core_gram[at] + gram[at, k]

    def c_rows(side, part):
        return pl.ds(128 // PARTS * part + 64 // PARTS * side, 64 // PARTS)

    def c2_copy(side, part):
        rows = c_rows(side, part)
        return remote(
            core_gram.at[(x + 2) % 4, rows], from_c1.at[rows], c2_send, c2_recv.at[part],
            x_sides[side],
        )

    def c3_copy(side, part, late):
        rows = c_rows(side if late else 1 - side, part)
        return remote(
            core_gram.at[(x + distances[side]) % 4, rows], from_c2.at[side, rows],
            c3_send, c3_recv.at[part if late else 0], x_sides[side],
        )

    def c4_copy(j, slot, part):
        rows = pl.ds(128 // PARTS * part, 128 // PARTS)
        return remote(
            final.at[j, rows], out.at[pl.ds(pl.multiple_of(slot * 128 + 128 // PARTS * part, 8), 128 // PARTS)],
            c4_send.at[j], c4_recv.at[slot], owners[j],
        )

    def c4_both(j):
        return remote(
            final.at[j], out.at[pl.ds(j * 128, 128)], c4_send.at[j], c4_recv.at[j], owners[j]
        )

    def own_copy(j):
        return pltpu.make_async_copy(final.at[j], out.at[pl.ds(j * 128, 128)], c4_send.at[j])

    combine(2)
    for part in range(PARTS):
        for side in range(2):
            c2_copy(side, part).start()
    for side in range(2):
        combine(distances[side])
        for part in range(PARTS):
            c3_copy(side, part, 0).start()
    combine(0)
    for part in range(PARTS):
        arrived(from_c1.at[pl.ds(0, 128 // PARTS)], c2_recv.at[part])
        for side in range(2):
            at, rows = (x + distances[side]) % 4, c_rows(side, part)
            core_gram[at, rows] = core_gram[at, rows] + from_c1[rows]
            c3_copy(side, part, 1).start()
    left_here(theirs, d_send)
    left_here(mine.at[2], x1_send)
    left_here(from_x2, x2_send)
    left_here(theirs, near_send)
    left_here(from_x2, far_send)
    for part in range(PARTS):
        size = 256 // PARTS + (256 if part == 0 else 0)
        arrived(from_core.at[0, pl.ds(0, size)], c3_recv.at[part])
        rows = pl.ds(128 // PARTS * part, 128 // PARTS)
        total = (core_gram[x, rows] + (from_c2[0, rows] + from_c2[1, rows])) * SCALE
        for j in range(2):
            final[j, rows] = total[:, j * 128:(j + 1) * 128]
        for j in range(2):
            @pl.when(2 * k + j != z)
            def _():
                c4_copy(j, z % 2, part).start()

            if part == PARTS - 1:
                @pl.when(2 * k + j == z)
                def _():
                    own_copy(j).start()

    left_here(core_gram, c1_send)
    left_here(from_c1, c2_send)
    left_here(from_c2, c3_send)
    for j in range(2):
        @pl.when(2 * k + j != z)
        def _():
            c4_both(j).wait()

        @pl.when(2 * k + j == z)
        def _():
            own_copy(j).wait()


def shards(slab, sign_bits, sample_rows):
    dma = pltpu.SemaphoreType.DMA
    vmem = lambda *shape: pltpu.VMEM(shape, jnp.float32)
    return pl.pallas_call(
        kernel,
        out_shape=jax.ShapeDtypeStruct((256, 128), jnp.float32),
        in_specs=[
            pl.BlockSpec(memory_space=pltpu.HBM),
            pl.BlockSpec(memory_space=pltpu.HBM),
            pl.BlockSpec(memory_space=pltpu.HBM),
        ],
        out_specs=pl.BlockSpec(memory_space=pltpu.HBM),
        scratch_shapes=[
            pltpu.VMEM((8 * SLOTS,), jnp.int32),
            pltpu.VMEM((HEIGHT // WIDE, WIDE), jnp.int32),
            vmem(HEIGHT, WIDE),
            vmem(2 * NEGATED, WIDE),
            pltpu.VMEM((256, 256), jnp.bfloat16),
            pltpu.VMEM((8 * SLOTS,), jnp.int32),
            pltpu.SMEM((8 * SLOTS,), jnp.int32),
            vmem(4, SLOTS, WIDE),
            vmem(4, SLOTS, WIDE),
            vmem(4, SLOTS, WIDE),
            vmem(SLOTS, WIDE),
            vmem(GROUPS, 2, STEP, WIDE),
            vmem(GROUPS, 4, WIDE, STEP),
            vmem(4, SLOTS, WIDE),
            vmem(4, 2, 128, 256),
            vmem(4, 128, 256),
            vmem(128, 256),
            vmem(2, 128, 256),
            vmem(2, 128, 128),
            dma((10,)), dma(()), dma((GROUPS, 4)),
            *[dma((GROUPS,))] * 5,
            dma((4,)), dma((PARTS,)), dma((PARTS,)), dma((2,)), dma((2,)),
            *[dma(())] * 8,
        ],
        compiler_params=pltpu.CompilerParams(
            collective_id=0, has_side_effects=True, vmem_limit_bytes=56 * 1024 * 1024
        ),
        name="sketch",
    )(sample_rows, sign_bits.reshape(64, 128), slab)


def solution(mesh):
    return jax.shard_map(
        shards,
        mesh=mesh,
        in_specs=(P("rows", "cols"), P("rows"), P()),
        out_specs=P("rows", "cols"),
        check_vma=False,
    )
```

```python
import functools

import jax
import jax.numpy as jnp
from jax import lax
from jax.experimental import pallas as pl
from jax.experimental.pallas import tpu as pltpu
from jax.sharding import PartitionSpec as P

HEIGHT = 8192
SLOTS = 1024
GROUPS = 8
STEP = SLOTS // GROUPS
HALF = STEP // 2
PARTS = 8
PITCH = 264
NEGATED = HEIGHT // 256 * PITCH
WIDE = 128
MESH = pl.DeviceIdType.MESH
SCALE = 1.0 / (8 * SLOTS * 8 * HEIGHT)

ORDER = (
    (0, 0, 2), (0, 0, 1), (0, 1, 2), (0, 2, 2), (0, 0, 3), (1, 0, 0), (0, 3, 2), (1, 1, 0),
    (0, 4, 2), (1, 2, 0), (0, 1, 1), (0, 1, 3), (2, 0, 0), (1, 3, 0), (0, 2, 1), (0, 5, 2),
    (0, 3, 1), (0, 2, 3), (2, 0, 1), (0, 4, 1), (0, 6, 2), (1, 4, 0), (3, 0, 0), (0, 0, 0),
    (0, 3, 3), (2, 1, 0), (2, 1, 1), (0, 5, 1), (0, 6, 1), (0, 4, 3), (0, 1, 0), (3, 1, 0),
    (2, 2, 0), (0, 7, 2), (0, 2, 0), (2, 2, 1), (0, 3, 0), (3, 2, 0), (2, 3, 0), (2, 3, 1),
    (0, 5, 3), (0, 4, 0), (3, 3, 0), (4, 0, 0), (1, 5, 0), (0, 5, 0), (0, 6, 3), (0, 7, 1),
    (4, 1, 0), (1, 6, 0), (0, 6, 0), (2, 4, 0), (2, 4, 1), (3, 4, 0), (1, 7, 0), (4, 2, 0),
    (2, 5, 0), (4, 3, 0), (0, 7, 3), (2, 5, 1), (5, 0, 0), (3, 5, 0), (2, 6, 0), (5, 0, 1),
    (2, 6, 1), (3, 6, 0), (2, 7, 0), (2, 7, 1), (5, 1, 0), (5, 1, 1), (5, 2, 0), (5, 2, 1),
    (4, 4, 0), (0, 7, 0), (3, 7, 0), (5, 3, 0), (5, 3, 1), (4, 5, 0), (4, 6, 0), (4, 7, 0),
    (6, 1, 1), (5, 4, 0), (5, 4, 1), (5, 5, 0), (5, 5, 1), (5, 6, 0), (5, 6, 1), (5, 7, 0),
    (5, 7, 1), (6, 3, 1), (6, 5, 1), (6, 6, 0), (6, 7, 0),
)


def parity_of(bits):
    bits = bits ^ (bits >> 4)
    bits = bits ^ (bits >> 2)
    bits = bits ^ (bits >> 1)
    return bits & 1


def split(value):
    high = value.astype(jnp.bfloat16)
    low = (value - high.astype(jnp.float32)).astype(jnp.bfloat16)
    return high, low


def kernel(
    samples_in, bits_in, slab, out,
    samples, bits, raw, table, matrix, code_rows, codes, mine, theirs, from_core, from_x1, from_x2,
    ybuf, zbuf, gram, core_gram, from_c1, from_c2, final,
    load_sem, code_sem, d_recv, x1_recv, x2_recv, y_recv, z_recv, far_recv,
    c1_recv, c2_recv, c3_recv, c4_recv, c4_send,
    d_send, x1_send, x2_send, near_send, far_send, c1_send, c2_send, c3_send,
):
    row = lax.axis_index("rows")
    col = lax.axis_index("cols")
    x, k = row // 2, row % 2
    y, z = col // 4, col % 4
    partner = (row + 1 - 2 * k, col)
    x_sides = ((((x + 3) % 4) * 2 + k, col), (((x + 1) % 4) * 2 + k, col))
    y_sides = ((row, ((y + 3) % 4) * 4 + z), (row, ((y + 1) % 4) * 4 + z))
    z_sides = ((row, y * 4 + (z + 3) % 4), (row, y * 4 + (z + 1) % 4))
    owners = [(x * 2 + z // 2, y * 4 + 2 * k + j) for j in range(2)]

    loads = [
        pltpu.make_async_copy(bits_in, bits, load_sem.at[8]),
        pltpu.make_async_copy(samples_in, samples, load_sem.at[9]),
    ]
    for part in range(8):
        rows = pl.ds(part * 1024, 1024)
        loads.append(pltpu.make_async_copy(slab.at[rows], raw.at[rows], load_sem.at[part]))
    for load in (loads[0], loads[2], loads[1], *loads[3:]):
        load.start()

    barrier = pltpu.get_barrier_semaphore()
    for other in (partner, *x_sides, *y_sides, *z_sides):
        pl.semaphore_signal(barrier, inc=1, device_id=other, device_id_type=MESH)
    for j in range(2):
        @pl.when(2 * k + j != z)
        def _():
            pl.semaphore_signal(barrier, inc=1, device_id=owners[j], device_id_type=MESH)

    left = lax.broadcasted_iota(jnp.int32, (256, 256), 0)
    right = lax.broadcasted_iota(jnp.int32, (256, 256), 1)
    matrix[...] = (1 - 2 * parity_of(left & right)).astype(jnp.float32).astype(jnp.bfloat16)

    def inside(q):
        signs = [
            (1 - 2 * bits[pl.ds(2 * q + i, 1), :]).astype(jnp.float32).astype(jnp.bfloat16)
            for i in range(2)
        ]
        signed = matrix[...] * jnp.concatenate(signs, axis=1)
        start = q * 256
        high, low = split(raw[pl.ds(start, 256), :])
        both = jnp.dot(
            signed, jnp.concatenate([high, low], axis=1), preferred_element_type=jnp.float32
        )
        table[pl.ds(q * PITCH, 256), :] = both[:, :128] + both[:, 128:]

    code_copy = pltpu.make_async_copy(code_rows, codes, code_sem)
    loads[0].wait()
    ends = (1, 4, 8)
    for last, end in enumerate(ends):
        for part in range(0 if last == 0 else ends[last - 1], end):
            loads[2 + part].wait()
        for q in range(0 if last == 0 else 4 * ends[last - 1], 4 * end):
            inside(q)
        if last == 0:
            loads[1].wait()
            parity = parity_of((samples[...] // HEIGHT) & row)
            offset = samples[...] % HEIGHT
            code_rows[...] = offset + offset // 256 * (PITCH - 256) + NEGATED * parity
        if last == 1:
            code_copy.start()

    def across(t, carry):
        starts = [pl.multiple_of(q * PITCH + t * 8, 8) for q in range(32)]
        values = [table[pl.ds(start, 8), :] for start in starts]
        span = 1
        while span < 32:
            for base in range(0, 32, 2 * span):
                for i in range(base, base + span):
                    first, second = values[i], values[i + span]
                    values[i], values[i + span] = first + second, first - second
            span *= 2
        for start, value in zip(starts, values):
            table[pl.ds(start, 8), :] = value
            table[pl.ds(start + NEGATED, 8), :] = -value
        return carry

    lax.fori_loop(0, 32, across, 0)
    code_copy.wait()

    pl.semaphore_wait(barrier, 8 + (z // 2 - k) * (z // 2 - k))

    def gather(g, d, core, target):
        base = (((x + d) % 4) * 2 + core) * SLOTS + g * STEP

        def some(i, carry):
            at = base + i * 32
            to = pl.multiple_of(g * STEP + i * 32, 32)
            for u in range(32):
                target[d, pl.ds(to + u, 1), :] = table[pl.ds(codes[at + u], 1), :]
            return carry

        lax.fori_loop(0, STEP // 32, some, 0)

    def remote(source, target, send, recv, device):
        return pltpu.make_async_remote_copy(
            src_ref=source, dst_ref=target, send_sem=send, recv_sem=recv,
            device_id=device, device_id_type=MESH,
        )

    def slots(g):
        return pl.ds(g * STEP, STEP)

    def half(g, side):
        return pl.ds(g * STEP + side * HALF, HALF)

    distances = (3, 1)

    def core_copy(g, d):
        return remote(
            theirs.at[d, slots(g)], from_core.at[d, slots(g)], d_send, d_recv.at[g, d], partner
        )

    def x1_copy(g, side):
        rows = half(g, side)
        return remote(mine.at[2, rows], from_x1.at[rows], x1_send, x1_recv.at[g], x_sides[side])

    def x2_copy(g, side, late):
        part = side if late else 1 - side
        return remote(
            mine.at[distances[side], half(g, part)], from_x2.at[g, side, pl.ds(part * HALF, HALF)],
            x2_send, x2_recv.at[g], x_sides[side],
        )

    def z_near(g, side, part):
        own = zbuf.at[z, half(g, side if part == 0 else 1 - side)]
        return remote(own, own, near_send, (z_recv, far_recv)[part].at[g], z_sides[side])

    def y_near(g, side, part):
        own = ybuf.at[g, y, pl.ds(64 * (side if part == 0 else 1 - side), 64)]
        return remote(own, own, near_send, (y_recv, far_recv)[part].at[g], y_sides[side])

    def came(at, side):
        return ((at + 1) % 4, (at + 3) % 4)[side]

    def z_far(g, side):
        part = zbuf.at[came(z, side), half(g, side)]
        return remote(part, part, far_send, far_recv.at[g], z_sides[side])

    def y_far(g, side):
        part = ybuf.at[g, came(y, side), pl.ds(64 * side, 64)]
        return remote(part, part, far_send, far_recv.at[g], y_sides[side])

    def arrived(like, semaphore):
        remote(like, like, semaphore, semaphore, partner).wait_recv()

    def left_here(like, semaphore):
        remote(like, like, semaphore, semaphore, partner).wait_send()

    def take_rows(g, d):
        gather(g, d, 1 - k, theirs)
        core_copy(g, d).start()
        gather(g, d, k, mine)

    def send_x1(g, _):
        core_copy(g, 2).wait_recv()
        mine[2, slots(g)] = mine[2, slots(g)] + from_core[2, slots(g)]
        x1_copy(g, 0).start()
        x1_copy(g, 1).start()

    def send_x2_early(g, side):
        d = distances[side]
        core_copy(g, d).wait_recv()
        mine[d, slots(g)] = mine[d, slots(g)] + from_core[d, slots(g)]
        x2_copy(g, side, 0).start()

    def send_x2_late(g, _):
        arrived(from_x1.at[slots(g)], x1_recv.at[g])
        for side in range(2):
            d, rows = distances[side], half(g, side)
            mine[d, rows] = mine[d, rows] + from_x1[rows]
            x2_copy(g, side, 1).start()

    def send_yz(g, _):
        core_copy(g, 0).wait_recv()
        arrived(from_x2.at[g], x2_recv.at[g])
        rows = slots(g)
        block = (mine[0, rows] + from_core[0, rows]) + (from_x2[g, 0] + from_x2[g, 1])
        zbuf[z, rows] = block
        ybuf[g, y] = block.T
        for part in range(2):
            for side in range(2):
                z_near(g, side, part).start()
                y_near(g, side, part).start()

    def forward(g, which):
        arrived(from_x1.at[slots(g)], (y_recv, z_recv)[which].at[g])
        for side in range(2):
            (y_far, z_far)[which](g, side).start()

    def multiply(g, more):
        groups = (g,) if not more else (g - 1, g)
        for each in groups:
            arrived(from_x2.at[pl.ds(0, 2)], far_recv.at[each])
        rows = pl.ds(groups[0] * STEP, STEP * len(groups))
        right = []
        for h in range(2):
            high, low = split(
                jnp.concatenate([zbuf[2 * h, rows], zbuf[2 * h + 1, rows]], axis=1)
            )
            right.append(jnp.concatenate([high, low, high], axis=0))
        for m in range(2):
            high, low = split(
                jnp.concatenate(
                    [
                        jnp.concatenate([ybuf[each, 2 * m], ybuf[each, 2 * m + 1]], axis=0)
                        for each in groups
                    ],
                    axis=1,
                )
            )
            left = jnp.concatenate([high, high, low], axis=1)
            for h in range(2):
                value = jnp.dot(left, right[h], preferred_element_type=jnp.float32)
                for i in range(2):
                    part = value[i * 128:(i + 1) * 128]
                    if groups[0]:
                        part = part + gram[2 * m + i, h]
                    gram[2 * m + i, h] = part

    def c1_copy(d):
        at = (x + d) % 4
        return remote(gram.at[at, 1 - k], core_gram.at[at], c1_send, c1_recv.at[d], partner)

    def multiply_last(g):
        arrived(from_x2.at[pl.ds(0, 2)], far_recv.at[g])
        right = []
        for h in range(2):
            high, low = split(
                jnp.concatenate([zbuf[2 * h, slots(g)], zbuf[2 * h + 1, slots(g)]], axis=1)
            )
            right.append(jnp.concatenate([high, low, high], axis=0))
        for d in (2, 3, 1, 0):
            at = (x + d) % 4
            high, low = split(ybuf[g, at])
            left = jnp.concatenate([high, high, low], axis=1)
            for h in range(2):
                gram[at, h] = gram[at, h] + jnp.dot(
                    left, right[h], preferred_element_type=jnp.float32
                )
            c1_copy(d).start()

    steps = (take_rows, send_x1, send_x2_early, send_x2_late, send_yz, forward, multiply)
    for kind, group, side in ORDER[:-1]:
        steps[kind](group, side)
    multiply_last(GROUPS - 1)

    def combine(d):
        at = (x + d) % 4
        c1_copy(d).wait_recv()
        core_gram[at] = core_gram[at] + gram[at, k]

    def c_rows(side, part):
        return pl.ds(128 // PARTS * part + 64 // PARTS * side, 64 // PARTS)

    def c2_copy(side, part):
        rows = c_rows(side, part)
        return remote(
            core_gram.at[(x + 2) % 4, rows], from_c1.at[rows], c2_send, c2_recv.at[part],
            x_sides[side],
        )

    def c3_copy(side, part, late):
        rows = c_rows(side if late else 1 - side, part)
        return remote(
            core_gram.at[(x + distances[side]) % 4, rows], from_c2.at[side, rows],
            c3_send, c3_recv.at[part if late else 0], x_sides[side],
        )

    def c4_copy(j, slot, part):
        rows = pl.ds(128 // PARTS * part, 128 // PARTS)
        return remote(
            final.at[j, rows], out.at[pl.ds(pl.multiple_of(slot * 128 + 128 // PARTS * part, 8), 128 // PARTS)],
            c4_send.at[j], c4_recv.at[slot], owners[j],
        )

    def c4_both(j):
        return remote(
            final.at[j], out.at[pl.ds(j * 128, 128)], c4_send.at[j], c4_recv.at[j], owners[j]
        )

    def own_copy(j):
        return pltpu.make_async_copy(final.at[j], out.at[pl.ds(j * 128, 128)], c4_send.at[j])

    combine(2)
    for part in range(PARTS):
        for side in range(2):
            c2_copy(side, part).start()
    for side in range(2):
        combine(distances[side])
        for part in range(PARTS):
            c3_copy(side, part, 0).start()
    combine(0)
    for part in range(PARTS):
        arrived(from_c1.at[pl.ds(0, 128 // PARTS)], c2_recv.at[part])
        for side in range(2):
            at, rows = (x + distances[side]) % 4, c_rows(side, part)
            core_gram[at, rows] = core_gram[at, rows] + from_c1[rows]
            c3_copy(side, part, 1).start()
    left_here(theirs, d_send)
    left_here(mine.at[2], x1_send)
    left_here(from_x2, x2_send)
    left_here(theirs, near_send)
    left_here(from_x2, far_send)
    for part in range(PARTS):
        size = 256 // PARTS + (256 if part == 0 else 0)
        arrived(from_core.at[0, pl.ds(0, size)], c3_recv.at[part])
        rows = pl.ds(128 // PARTS * part, 128 // PARTS)
        total = (core_gram[x, rows] + (from_c2[0, rows] + from_c2[1, rows])) * SCALE
        for j in range(2):
            final[j, rows] = total[:, j * 128:(j + 1) * 128]
        for j in range(2):
            @pl.when(2 * k + j != z)
            def _():
                c4_copy(j, z % 2, part).start()

            if part == PARTS - 1:
                @pl.when(2 * k + j == z)
                def _():
                    own_copy(j).start()

    left_here(core_gram, c1_send)
    left_here(from_c1, c2_send)
    left_here(from_c2, c3_send)
    for j in range(2):
        @pl.when(2 * k + j != z)
        def _():
            c4_both(j).wait()

        @pl.when(2 * k + j == z)
        def _():
            own_copy(j).wait()


def shards(slab, sign_bits, sample_rows):
    dma = pltpu.SemaphoreType.DMA
    vmem = lambda *shape: pltpu.VMEM(shape, jnp.float32)
    return pl.pallas_call(
        kernel,
        out_shape=jax.ShapeDtypeStruct((256, 128), jnp.float32),
        in_specs=[
            pl.BlockSpec(memory_space=pltpu.HBM),
            pl.BlockSpec(memory_space=pltpu.HBM),
            pl.BlockSpec(memory_space=pltpu.HBM),
        ],
        out_specs=pl.BlockSpec(memory_space=pltpu.HBM),
        scratch_shapes=[
            pltpu.VMEM((8 * SLOTS,), jnp.int32),
            pltpu.VMEM((HEIGHT // WIDE, WIDE), jnp.int32),
            vmem(HEIGHT, WIDE),
            vmem(2 * NEGATED, WIDE),
            pltpu.VMEM((256, 256), jnp.bfloat16),
            pltpu.VMEM((8 * SLOTS,), jnp.int32),
            pltpu.SMEM((8 * SLOTS,), jnp.int32),
            vmem(4, SLOTS, WIDE),
            vmem(4, SLOTS, WIDE),
            vmem(4, SLOTS, WIDE),
            vmem(SLOTS, WIDE),
            vmem(GROUPS, 2, STEP, WIDE),
            vmem(GROUPS, 4, WIDE, STEP),
            vmem(4, SLOTS, WIDE),
            vmem(4, 2, 128, 256),
            vmem(4, 128, 256),
            vmem(128, 256),
            vmem(2, 128, 256),
            vmem(2, 128, 128),
            dma((10,)), dma(()), dma((GROUPS, 4)),
            *[dma((GROUPS,))] * 5,
            dma((4,)), dma((PARTS,)), dma((PARTS,)), dma((2,)), dma((2,)),
            *[dma(())] * 8,
        ],
        compiler_params=pltpu.CompilerParams(
            collective_id=0, has_side_effects=True, vmem_limit_bytes=56 * 1024 * 1024
        ),
        name="sketch",
    )(sample_rows, sign_bits.reshape(64, 128), slab)


def solution(mesh):
    return jax.shard_map(
        shards,
        mesh=mesh,
        in_specs=(P("rows", "cols"), P("rows"), P()),
        out_specs=P("rows", "cols"),
        check_vma=False,
    )
```
